1024 devices in a mesh: lon: 64 (over z_hi, y, core), lat: 16 (over x, z_lo).
Axes of the slice: x: 8, y: 8, z: 8 (z_hi: 4, z_lo: 2; z = z_hi * 2 + z_lo), core: 2. Of those that a mesh axis runs over, the one named last changes fastest.
Arguments:
- depth_init: float32 [4096, 8192], P('lat', 'lon'), may hold values from 0.5 to 2.5
- ground: float32 [4096, 8192], P('lat', 'lon'), may hold values from -4 to 4
- roughness: float32 [4096, 8192], P('lat', 'lon'), may hold values from 0.02 to 0.12
- river_init: float32 [4096, 8192], P('lat', 'lon'), may hold values from 0.5 to 4.5
- reach_mask: int32 [4096, 64], P('lat', 'lon'), may hold values from 0 to 1, as said below
- width_class: int32 [4096, 8192], P('lat', 'lon'), may hold values from 0 to 7
- bank_class: int32 [4096, 8192], P('lat', 'lon'), may hold values from 0 to 7
Outputs:
- flood_depth: float32 [4096, 8192], P('lat', 'lon')
- river_depth: float32 [4096, 8192], P('lat', 'lon')
- flow_east: float32 [4096, 8192], P('lat', 'lon')
- flow_north: float32 [4096, 8192], P('lat', 'lon')
The draws below stay inside these ranges and needn't reach their ends.
Inputs may be any that keep to these rules, and one draw needn't show every extreme that they name: Call the 256 rows of one lat index and one lon index of reach_mask a tile. A tile has at most 64 channelled reaches, and some tile exactly 64. A tile with more than 32 has 34 or more, and lies four or more lon indices (around the cycle) from any other such tile of the same lat index; every other tile has at most 16, and some tile beside a full one exactly that many.
All inputs are finite; a program needn't handle non-finite values.
Results may differ from the reference program's by a relative error of at most 0.00002.
Values sent between devices are 32-bit elements; how exact they have to be, the bound alone decides.
A program may use at most 32 MiB of HBM per device.

```python
import math
import jax
import jax.numpy as jnp

REACH = 128
CY = 256
SUB = 8
STEPS = 4
NY = 4096
NX = 8192
N_LON = 64
N_LAT = 16


def draw_reach_mask(key, part):
    most_slots = CY // 4
    home_slots = CY // 8
    spare_slots = CY // 16
    subkeys = jax.random.split(jax.random.fold_in(key, 17), 3)
    lon_number = jnp.arange(N_LON)[None, :]
    lat_number = jnp.arange(N_LAT)[:, None]
    crowded = (lon_number + lat_number) % 4 == 0
    loaded_count = jax.random.randint(subkeys[0], (N_LAT, N_LON), home_slots + 2, most_slots + 1)
    sparse_count = jax.random.randint(subkeys[1], (N_LAT, N_LON), 0, home_slots - spare_slots + 1)
    counts = jnp.where(crowded, loaded_count, sparse_count)
    counts = counts.at[0, 0].set(most_slots).at[0, 1].set(home_slots - spare_slots)
    scores = jax.random.randint(subkeys[2], (N_LAT, N_LON, CY), 0, 1 << 20) * CY + jnp.arange(CY)[None, None, :]
    row_ranks = jnp.argsort(jnp.argsort(scores, axis=-1), axis=-1)
    chosen = (row_ranks < counts[:, :, None]).astype(jnp.int32)
    return jnp.transpose(chosen, (0, 2, 1)).reshape(N_LAT * CY, N_LON)


def place_ends(entries, stream_key, smallest, top_value):
    shape = entries.shape
    spot = [jax.random.randint(jax.random.fold_in(stream_key, axis), (), 0, shape[axis]) for axis in range(len(shape))]
    entries = entries.at[tuple(spot)].set(smallest)
    longest = shape.index(max(shape))
    spot[longest] = (spot[longest] + 1) % shape[longest]
    return entries.at[tuple(spot)].set(top_value)


def levels(key, extent, shards, low, largest):
    def one(position, blocks):
        heights = jax.random.uniform(jax.random.fold_in(jax.random.fold_in(key, 6), position), (blocks,), jnp.float32, low / len(shards), largest / len(shards))
        return jnp.repeat(jnp.exp(heights), extent[position] // blocks).reshape((-1,) + (1,) * (len(extent) - position - 1))

    level = one(*shards[0])
    for cut in shards[1:]:
        level = level * one(*cut)
    return level


def noise(key, shape, scale, limit, pieces=(), held_as=jnp.bfloat16):
    level = levels(key, shape, pieces, -0.22, 0.18) if pieces else 1.0
    array = jax.random.normal(key, shape, jnp.float32) * scale * level
    return jnp.minimum(jnp.maximum(array, -limit), limit).astype(held_as)


def setup_inputs(seed: int = 0) -> dict:
    arg_keys = jax.random.split(jax.random.key(seed), 8)
    depth_init = jnp.clip(0.5 + 2.0 * jax.random.uniform(arg_keys[0], (NY, NX), jnp.float32) ** levels(arg_keys[0], (NY, NX), ((0, 16), (1, 64)), -0.2, 0.2), 0.5, 2.5)
    ground = noise(arg_keys[1], (NY, NX), 1.0, 4.0, ((0, 16), (1, 64)), jnp.float32)
    roughness = jnp.clip(jnp.exp(math.log(0.12) - 1.7917595 * jax.random.uniform(arg_keys[2], (NY, NX), jnp.float32) ** levels(arg_keys[2], (NY, NX), ((0, 16), (1, 64)), -0.2, 0.2)), 0.02, 0.12)
    river_init = jnp.clip(0.5 + 4.0 * jax.random.uniform(arg_keys[3], (NY, NX), jnp.float32) ** levels(arg_keys[3], (NY, NX), ((0, 16), (1, 64)), -0.2, 0.2), 0.5, 4.5)
    reach_mask = draw_reach_mask(jax.random.fold_in(arg_keys[7], 71), 0)
    width_class = place_ends(jax.random.randint(arg_keys[5], (NY, NX), 0, 8), jax.random.fold_in(arg_keys[5], 1), 0, 7).astype(jnp.int32)
    bank_class = place_ends(jax.random.randint(arg_keys[6], (NY, NX), 0, 8), jax.random.fold_in(arg_keys[6], 1), 0, 7).astype(jnp.int32)
    return {"depth_init": depth_init, "ground": ground, "roughness": roughness, "river_init": river_init, "reach_mask": reach_mask, "width_class": width_class, "bank_class": bank_class}


GRAVITY = 9.81
CELL_SIZE = 90.0
TIME_STEP = 10.0
SHALLOW = 0.1
EXCHANGE = 0.01
CHANNEL_MANNING = 0.035


def face_flow(current, surface_from, surface_to, ground_from, ground_to, friction, breadth, duration):
    height = jnp.maximum(surface_from, surface_to) - jnp.maximum(ground_from, ground_to)
    driven = current - GRAVITY * duration * breadth * height * (surface_to - surface_from) / CELL_SIZE
    resisted = 1.0 + GRAVITY * duration * friction * jnp.abs(current) / (height * height + SHALLOW * SHALLOW) ** (7.0 / 6.0)
    return driven / resisted


def reach_update(river_bed, channel_width, safe_width, river_depth, discharge, surface):
    duration = TIME_STEP / SUB
    breadth = 0.5 * (channel_width[:, :-1] + channel_width[:, 1:])
    safe_breadth = 0.5 * (safe_width[:, :-1] + safe_width[:, 1:])
    friction = CHANNEL_MANNING * CHANNEL_MANNING / safe_breadth
    closed = jnp.zeros_like(river_depth[:, :1])
    gathered = jnp.zeros_like(river_depth)
    for substep in range(SUB):
        water_level = river_bed + river_depth
        interior = face_flow(discharge[:, :-1], water_level[:, :-1], water_level[:, 1:], river_bed[:, :-1], river_bed[:, 1:], friction, breadth, duration)
        discharge = jnp.concatenate([interior, closed], axis=1)
        inflow = jnp.concatenate([closed, interior], axis=1)
        transfer = EXCHANGE * (water_level - surface)
        river_depth = river_depth + duration * ((inflow - discharge) / (safe_width * CELL_SIZE) - transfer)
        gathered = gathered + duration * transfer
    return river_depth, discharge, gathered


def reference(depth_init, ground, roughness, river_init, reach_mask, width_class, bank_class):
    row_count, col_count = ground.shape
    channel_width = 8.0 + 9.0 * width_class.astype(jnp.float32)
    river_bed = ground - (1.0 + 0.5 * bank_class.astype(jnp.float32))
    channelled = jnp.repeat(reach_mask, REACH, axis=1) > 0
    open_north = (jnp.arange(row_count) < row_count - 1)[:, None]

    def as_reaches(field):
        return field.reshape(row_count * N_LON, REACH)

    def as_cells(field):
        return field.reshape(row_count, col_count)

    flood = depth_init
    river_depth = river_init
    discharge = jnp.zeros((row_count, col_count), jnp.float32)
    flow_east = jnp.zeros((row_count, col_count), jnp.float32)
    flow_north = jnp.zeros((row_count, col_count), jnp.float32)
    zero_row = jnp.zeros((1, col_count), jnp.float32)
    for repeat in range(STEPS):
        surface = ground + flood
        flow_east = face_flow(flow_east, surface, jnp.roll(surface, -1, 1), ground, jnp.roll(ground, -1, 1),
                              roughness * jnp.roll(roughness, -1, 1), 1.0, TIME_STEP)
        north_flux = face_flow(flow_north, surface, jnp.roll(surface, -1, 0), ground, jnp.roll(ground, -1, 0),
                               roughness * jnp.roll(roughness, -1, 0), 1.0, TIME_STEP)
        flow_north = jnp.where(open_north, north_flux, 0.0)
        from_west = jnp.roll(flow_east, 1, 1)
        from_south = jnp.concatenate([zero_row, flow_north[:-1]], axis=0)
        flooded = flood + TIME_STEP / CELL_SIZE * (from_west - flow_east + from_south - flow_north)
        new_river, new_discharge, gathered = reach_update(
            as_reaches(river_bed), as_reaches(channel_width), as_reaches(channel_width),
            as_reaches(river_depth), as_reaches(discharge), as_reaches(surface))
        flood = flooded + jnp.where(channelled, as_cells(gathered) * channel_width / CELL_SIZE, 0.0)
        river_depth = jnp.where(channelled, as_cells(new_river), river_depth)
        discharge = jnp.where(channelled, as_cells(new_discharge), discharge)
    return flood, river_depth, flow_east, flow_north
```

```python
import functools
import math

import jax
import jax.numpy as jnp
from jax import lax
from jax.experimental import pallas as pl
from jax.experimental.pallas import tpu as pltpu
from jax.sharding import PartitionSpec as P

MESH = pl.DeviceIdType.MESH
F32 = jnp.float32
SUB = 8
STEPS = 4
ROWS = 256
COLS = 128
HALO = 24
WIDE = COLS + 2 * HALO
SEG = WIDE // 8
LANES = 128
TILES = 3
DEPTH, GROUND, ROUGH, RIVER, WIDTH, BED = range(6)
FROM_S, FROM_N, FROM_SW, FROM_SE, FROM_NW, FROM_NE = range(6)

GRAVITY = 9.81
CELL_SIZE = 90.0
TIME_STEP = 10.0
SHALLOW = 0.1
EXCHANGE = 0.01
CHANNEL_MANNING = 0.035
SHORT_STEP = TIME_STEP / SUB
POWER = -7.0 / 6.0 / math.log(2.0)


def exchange_kernel(
    n_lon,
    n_lat,
    depth_hbm,
    ground_hbm,
    rough_hbm,
    river_hbm,
    width_hbm,
    bank_hbm,
    mask_hbm,
    ext,
    sides,
    strips,
    own_mask,
    floats,
    ints,
    mask_in,
    top,
    bottom,
    load_sem,
    send_sem,
    recv_sem,
):
    lon = lax.axis_index("lon")
    lat = lax.axis_index("lat")
    east = lax.rem(lon + 1, n_lon)
    west = lax.rem(lon + n_lon - 1, n_lon)
    north = lax.rem(lat + 1, n_lat)
    south = lax.rem(lat + n_lat - 1, n_lat)
    around = [
        (east, lat),
        (west, lat),
        (lon, north),
        (lon, south),
        (east, north),
        (west, north),
        (east, south),
        (west, south),
    ]
    around = [{"lon": a, "lat": b} for a, b in around]
    barrier = pltpu.get_barrier_semaphore()
    for device in around:
        pl.semaphore_signal(barrier, inc=1, device_id=device, device_id_type=MESH)

    loads = []
    for number, (source, target) in enumerate(
        [
            (ground_hbm, floats.at[GROUND]),
            (bank_hbm, ints.at[0]),
            (width_hbm, ints.at[1]),
            (river_hbm, floats.at[RIVER]),
            (depth_hbm, floats.at[DEPTH]),
            (rough_hbm, floats.at[ROUGH]),
            (mask_hbm, mask_in),
        ]
    ):
        copy = pltpu.make_async_copy(source, target, load_sem.at[number])
        copy.start()
        loads.append(copy)

    def place(field, values):
        for tile in range(2):
            ext[field, tile, HALO : HALO + COLS, :] = values[tile * LANES : (tile + 1) * LANES, :].T
        top[field] = values[0:8, :]
        bottom[field] = values[ROWS - 8 : ROWS, :]

    loads[0].wait()
    ground = floats[GROUND]
    place(GROUND, ground)
    loads[1].wait()
    place(BED, ground - (1.0 + 0.5 * ints[0].astype(F32)))
    loads[2].wait()
    place(WIDTH, 8.0 + 9.0 * ints[1].astype(F32))
    loads[3].wait()
    place(RIVER, floats[RIVER])
    loads[4].wait()
    place(DEPTH, floats[DEPTH])
    loads[5].wait()
    place(ROUGH, floats[ROUGH])
    loads[6].wait()
    for tile in range(2):
        own_mask[tile] = jnp.broadcast_to(mask_in[tile : tile + 1, :].astype(F32), (8, LANES))
    top[6] = own_mask[0]
    bottom[6] = own_mask[1]

    pl.semaphore_wait(barrier, len(around))
    fields = pl.ds(0, 6)
    both = pl.ds(0, 2)
    sends = [
        (
            ext.at[fields, both, pl.ds(COLS, HALO), :],
            ext.at[fields, both, pl.ds(0, HALO), :],
            around[0],
        ),
        (
            ext.at[fields, both, pl.ds(HALO, HALO), :],
            ext.at[fields, both, pl.ds(HALO + COLS, HALO), :],
            around[1],
        ),
        (bottom, strips.at[FROM_SW], around[4]),
        (bottom, strips.at[FROM_SE], around[5]),
        (top, strips.at[FROM_NW], around[6]),
        (top, strips.at[FROM_NE], around[7]),
        (bottom, strips.at[FROM_S], around[2]),
        (top, strips.at[FROM_N], around[3]),
        (own_mask, sides.at[0], around[0]),
        (own_mask, sides.at[1], around[1]),
    ]
    copies = []
    for number, (source, target, device) in enumerate(sends):
        copy = pltpu.make_async_remote_copy(
            src_ref=source,
            dst_ref=target,
            send_sem=send_sem.at[number],
            recv_sem=recv_sem.at[number],
            device_id=device,
            device_id_type=MESH,
        )
        copy.start()
        copies.append(copy)
    for copy in copies:
        copy.wait()


def quotient(current, height, drop, friction, drive):
    power = jnp.exp2(POWER * jnp.log(height * height + SHALLOW * SHALLOW))
    resisted = 1.0 + friction * jnp.abs(current) * power
    return (current - drive * (height * drop)) / resisted


def flow_kernel(
    n_lat,
    ext,
    sides,
    strips,
    own_mask,
    flood_out,
    river_out,
    east_out,
    north_out,
    third,
    g,
    fl,
    sur,
    q_east,
    q_north,
    e_base,
    e_fric,
    n_base,
    n_fric,
    level,
    flux,
    bed,
    r_base,
    r_drive,
    r_fric,
    r_inv,
    give,
    total,
    spread,
):
    lat = lax.axis_index("lat")
    lane = lax.broadcasted_iota(jnp.int32, (8, LANES), 1)
    sublane = lax.broadcasted_iota(jnp.int32, (8, LANES), 0)
    last_lane = lane == LANES - 1
    first_lane = lane == 0

    ones = jnp.full((112, LANES), 1.0, F32)
    for field in range(6):
        for from_n, from_s, source, target, count in (
            (FROM_NW, FROM_SW, COLS - HALO, 0, HALO),
            (FROM_N, FROM_S, 0, HALO, COLS),
            (FROM_NE, FROM_SE, 0, HALO + COLS, HALO),
        ):
            block = jnp.concatenate([strips[from_n, field], ones, strips[from_s, field]], axis=0).T
            third[field, target : target + count, :] = block[source : source + count, :]

    def load(field, tile, j):
        if tile < 2:
            return ext[field, tile, pl.ds(j, 8, stride=SEG), :]
        return third[field, pl.ds(j, 8, stride=SEG), :]

    def after(values, j):
        return values[j + 1] if j + 1 < SEG else pltpu.roll(values[0], 7, 0)

    def before(values, j):
        return values[j - 1] if j else pltpu.roll(values[SEG - 1], 1, 0)

    def northward(values, tile):
        here = pltpu.roll(values[tile], LANES - 1, 1)
        there = pltpu.roll(values[(tile + 1) % TILES], LANES - 1, 1)
        return jnp.where(last_lane, there, here)

    def southward(values, tile):
        here = pltpu.roll(values[tile], 1, 1)
        there = pltpu.roll(values[(tile + TILES - 1) % TILES], 1, 1)
        return jnp.where(first_lane, there, here)

    near = lane < 64
    masks = []
    for tile in range(2):
        masks.append((sides[0, tile], own_mask[tile], sides[1, tile]))
    masks.append(
        tuple(
            jnp.where(near, strips[a, 6], strips[b, 6])
            for a, b in ((FROM_NW, FROM_SW), (FROM_N, FROM_S), (FROM_NE, FROM_SE))
        )
    )
    for tile in range(TILES):
        grounds = [load(GROUND, tile, j) for j in range(SEG)]
        roughs = [load(ROUGH, tile, j) for j in range(SEG)]
        for j in range(SEG):
            g[tile, j] = grounds[j]
            fl[tile, j] = load(DEPTH, tile, j)
            e_base[tile, j] = jnp.maximum(grounds[j], after(grounds, j))
            e_fric[tile, j] = (GRAVITY * TIME_STEP) * (roughs[j] * after(roughs, j))
            n_fric[tile, j] = roughs[j]
            q_east[tile, j] = jnp.zeros((8, LANES), F32)
            q_north[tile, j] = jnp.zeros((8, LANES), F32)
        beds = [load(BED, tile, j) for j in range(SEG)]
        widths = [load(WIDTH, tile, j) for j in range(SEG)]
        for j in range(SEG):
            column = sublane * SEG + j
            closed = (column == HALO - 1) | (column == HALO + COLS - 1) | (column == WIDE - 1)
            breadth = 0.5 * (widths[j] + after(widths, j))
            bed[tile, j] = beds[j]
            level[tile, j] = beds[j] + load(RIVER, tile, j)
            flux[tile, j] = jnp.zeros((8, LANES), F32)
            r_base[tile, j] = jnp.maximum(beds[j], after(beds, j))
            r_drive[tile, j] = jnp.where(
                closed, 0.0, (GRAVITY * SHORT_STEP / CELL_SIZE) * breadth
            )
            r_fric[tile, j] = (
                GRAVITY * SHORT_STEP * CHANNEL_MANNING * CHANNEL_MANNING
            ) / breadth
            r_inv[tile, j] = SHORT_STEP / (CELL_SIZE * widths[j])
            mask = jnp.where(
                column < HALO,
                masks[tile][0],
                jnp.where(column < HALO + COLS, masks[tile][1], masks[tile][2]),
            )
            give[tile, j] = mask * widths[j] * (SHORT_STEP * EXCHANGE / CELL_SIZE)
    for j in range(SEG):
        grounds = [g[tile, j] for tile in range(TILES)]
        roughs = [n_fric[tile, j] for tile in range(TILES)]
        for tile in range(TILES):
            n_base[tile, j] = jnp.maximum(grounds[tile], northward(grounds, tile))
            n_fric[tile, j] = (GRAVITY * TIME_STEP) * (roughs[tile] * northward(roughs, tile))

    drive = GRAVITY * TIME_STEP / CELL_SIZE
    n_drive = [
        jnp.full((8, LANES), drive, F32),
        jnp.where(last_lane & (lat == n_lat - 1), 0.0, drive),
        jnp.where(last_lane & (lat == 0), 0.0, drive),
    ]

    for step in range(STEPS):
        tiles = TILES if step < STEPS - 1 else 2
        for tile in range(TILES):
            for j in range(SEG):
                sur[tile, j] = g[tile, j] + fl[tile, j]
                total[tile, j] = jnp.zeros((8, LANES), F32)

        for tile in range(tiles):
            surfaces = [sur[tile, j] for j in range(SEG)]
            for j in range(SEG):
                east = after(surfaces, j)
                q_east[tile, j] = quotient(
                    q_east[tile, j],
                    jnp.maximum(surfaces[j], east) - e_base[tile, j],
                    east - surfaces[j],
                    e_fric[tile, j],
                    drive,
                )
        for j in range(SEG):
            surfaces = [sur[tile, j] for tile in range(TILES)]
            for tile in range(TILES):
                north = northward(surfaces, tile)
                q_north[tile, j] = quotient(
                    q_north[tile, j],
                    jnp.maximum(surfaces[tile], north) - n_base[tile, j],
                    north - surfaces[tile],
                    n_fric[tile, j],
                    n_drive[tile],
                )

        def substep(_, carry):
            for tile in range(tiles):
                first = level[tile, 0]
                first_flux = None
                here = first
                last_flux = None
                for j in range(SEG):
                    there = level[tile, j + 1] if j + 1 < SEG else pltpu.roll(first, 7, 0)
                    out = quotient(
                        flux[tile, j],
                        jnp.maximum(here, there) - r_base[tile, j],
                        there - here,
                        r_fric[tile, j],
                        r_drive[tile, j],
                    )
                    flux[tile, j] = out
                    total[tile, j] += here
                    if j:
                        level[tile, j] = (
                            here
                            - (SHORT_STEP * EXCHANGE) * (here - sur[tile, j])
                            + (last_flux - out) * r_inv[tile, j]
                        )
                    else:
                        first_flux = out
                    last_flux = out
                    here = there
                level[tile, 0] = (
                    first
                    - (SHORT_STEP * EXCHANGE) * (first - sur[tile, 0])
                    + (pltpu.roll(last_flux, 1, 0) - first_flux) * r_inv[tile, 0]
                )
            return carry

        lax.fori_loop(0, SUB, substep, 0)

        for j in range(SEG):
            norths = [q_north[tile, j] for tile in range(TILES)]
            for tile in range(tiles):
                east = q_east[tile, j]
                west = q_east[tile, j - 1] if j else pltpu.roll(q_east[tile, SEG - 1], 1, 0)
                flooded = fl[tile, j] + (TIME_STEP / CELL_SIZE) * (
                    west - east + southward(norths, tile) - norths[tile]
                )
                fl[tile, j] = flooded + give[tile, j] * (total[tile, j] - SUB * sur[tile, j])

    own = pl.ds(HALO, COLS)
    for number, (source, target) in enumerate(
        ((fl, flood_out), (level, river_out), (q_east, east_out), (q_north, north_out))
    ):
        for tile in range(2):
            for j in range(SEG):
                value = source[tile, j]
                if number == 1:
                    column = sublane * SEG + j
                    value = value - bed[tile, j]
                    before_all = load(RIVER, tile, j)
                    value = jnp.where(own_mask[tile] > 0.0, value, before_all)
                spread[tile, pl.ds(j, 8, stride=SEG), :] = value
            target[tile * LANES : (tile + 1) * LANES, :] = spread[tile, own, :].T


def body(n_lon, n_lat, depth_init, ground, roughness, river_init, reach_mask, width_class, bank_class):
    mask = reach_mask.reshape(2, LANES)
    field = (ROWS, COLS)
    anywhere = pl.BlockSpec(memory_space=pl.ANY)
    near = pl.BlockSpec(memory_space=pltpu.VMEM)
    ext, sides, strips, own_mask = pl.pallas_call(
        functools.partial(exchange_kernel, n_lon, n_lat),
        out_shape=(
            jax.ShapeDtypeStruct((6, 2, WIDE, LANES), F32),
            jax.ShapeDtypeStruct((2, 2, 8, LANES), F32),
            jax.ShapeDtypeStruct((6, 7, 8, LANES), F32),
            jax.ShapeDtypeStruct((2, 8, LANES), F32),
        ),
        in_specs=[anywhere] * 7,
        out_specs=(near,) * 4,
        scratch_shapes=[
            pltpu.VMEM((4, ROWS, COLS), F32),
            pltpu.VMEM((2, ROWS, COLS), jnp.int32),
            pltpu.VMEM((2, LANES), jnp.int32),
            pltpu.VMEM((7, 8, LANES), F32),
            pltpu.VMEM((7, 8, LANES), F32),
            pltpu.SemaphoreType.DMA((7,)),
            pltpu.SemaphoreType.DMA((10,)),
            pltpu.SemaphoreType.DMA((10,)),
        ],
        compiler_params=pltpu.CompilerParams(collective_id=0, has_side_effects=True),
        name="exchange",
    )(depth_init, ground, roughness, river_init, width_class, bank_class, mask)
    state = pltpu.VMEM((TILES, SEG, 8, LANES), F32)
    return pl.pallas_call(
        functools.partial(flow_kernel, n_lat),
        out_shape=(jax.ShapeDtypeStruct(field, F32),) * 4,
        in_specs=[near] * 4,
        out_specs=(near,) * 4,
        scratch_shapes=[pltpu.VMEM((6, WIDE, LANES), F32)]
        + [state] * 18
        + [pltpu.VMEM((2, WIDE, LANES), F32)],
        name="flow",
    )(ext, sides, strips, own_mask)


def solution(mesh):
    placed = P("lat", "lon")
    return jax.shard_map(
        functools.partial(body, mesh.shape["lon"], mesh.shape["lat"]),
        mesh=mesh,
        in_specs=(placed,) * 7,
        out_specs=(placed,) * 4,
        check_vma=False,
    )
```

```python
import functools
import math

import jax
import jax.numpy as jnp
from jax import lax
from jax.experimental import pallas as pl
from jax.experimental.pallas import tpu as pltpu
from jax.sharding import PartitionSpec as P

MESH = pl.DeviceIdType.MESH
F32 = jnp.float32
SUB = 8
STEPS = 4
ROWS = 256
COLS = 128
HALO = 24
WIDE = COLS + 2 * HALO
LANES = 128
STRIP = 40
BAND = 96
STARTS = (0, 8, 16, 16)
DEPTH, GROUND, ROUGH, RIVER, WIDTH, BED = range(6)
FROM_S, FROM_N, FROM_SW, FROM_SE, FROM_NW, FROM_NE = range(6)
FLOOD, LEVEL, EAST, NORTH, FLUX = range(5)

GRAVITY = 9.81
CELL_SIZE = 90.0
TIME_STEP = 10.0
SHALLOW = 0.1
EXCHANGE = 0.01
CHANNEL_MANNING = 0.035
SHORT_STEP = TIME_STEP / SUB
POWER = -7.0 / 6.0 / math.log(2.0)
DRIVE = GRAVITY * TIME_STEP / CELL_SIZE

STATE = 5
SCRATCH = 17
REGISTERS = 32
VMEM_LIMIT = 24 << 20


def quotient(current, height, drop, friction, drive):
    power = jnp.exp2(POWER * jnp.log(height * height + SHALLOW * SHALLOW))
    resisted = 1.0 + friction * jnp.abs(current) * power
    return (current - drive * (height * drop)) / resisted


class Zone:
    def __init__(self, refs, sizes, partners):
        self.sizes = sizes
        self.partners = partners
        self.base = [sum(sizes[:t]) for t in range(len(sizes))]
        self.state = refs[:STATE]
        (
            self.g,
            self.sur,
            self.e_base,
            self.e_fric,
            self.n_base,
            self.n_fric,
            self.r_base,
            self.r_drive,
            self.r_fric,
            self.r_inv,
            self.give,
            self.total,
        ) = refs[STATE:]
        self.lane = lax.broadcasted_iota(jnp.int32, (8, LANES), 1)
        self.sublane = lax.broadcasted_iota(jnp.int32, (8, LANES), 0)

    def column(self, tile, j):
        return self.sublane * self.sizes[tile] + j

    def northward(self, read, tile):
        here = pltpu.roll(read(tile), LANES - 1, 1)
        if self.partners[tile] == tile:
            return here
        there = pltpu.roll(read(self.partners[tile]), LANES - 1, 1)
        return jnp.where(self.lane == LANES - 1, there, here)

    def southward(self, read, tile):
        here = pltpu.roll(read(tile), 1, 1)
        if self.partners[tile] == tile:
            return here
        there = pltpu.roll(read(self.partners[tile]), 1, 1)
        return jnp.where(self.lane == 0, there, here)

    def prepare(self, tile, load, closed, mask):
        size, base = self.sizes[tile], self.base[tile]

        def after(values, j):
            return values[j + 1] if j + 1 < size else pltpu.roll(values[0], 7, 0)

        grounds = [load(GROUND, j) for j in range(size)]
        roughs = [load(ROUGH, j) for j in range(size)]
        beds = [load(BED, j) for j in range(size)]
        widths = [load(WIDTH, j) for j in range(size)]
        for j in range(size):
            at = base + j
            column = self.column(tile, j)
            self.g[at] = grounds[j]
            self.e_base[at] = jnp.maximum(grounds[j], after(grounds, j))
            self.e_fric[at] = (GRAVITY * TIME_STEP) * (roughs[j] * after(roughs, j))
            self.n_fric[at] = roughs[j]
            breadth = 0.5 * (widths[j] + after(widths, j))
            self.r_base[at] = jnp.maximum(beds[j], after(beds, j))
            self.r_drive[at] = jnp.where(
                closed(column), 0.0, (GRAVITY * SHORT_STEP / CELL_SIZE) * breadth
            )
            self.r_fric[at] = (
                GRAVITY * SHORT_STEP * CHANNEL_MANNING * CHANNEL_MANNING
            ) / breadth
            self.r_inv[at] = SHORT_STEP / (CELL_SIZE * widths[j])
            self.give[at] = mask(column) * widths[j] * (SHORT_STEP * EXCHANGE / CELL_SIZE)

    def prepare_north(self, tiles):
        for j in range(self.sizes[tiles[0]]):
            grounds = {t: self.g[self.base[t] + j] for t in tiles}
            roughs = {t: self.n_fric[self.base[t] + j] for t in tiles}
            for t in tiles:
                at = self.base[t] + j
                self.n_base[at] = jnp.maximum(grounds[t], self.northward(grounds.get, t))
                self.n_fric[at] = (GRAVITY * TIME_STEP) * (
                    roughs[t] * self.northward(roughs.get, t)
                )

    def begin(self, tile, load):
        for j in range(self.sizes[tile]):
            at = self.base[tile] + j
            self.state[FLOOD][at] = load(DEPTH, j)
            self.state[LEVEL][at] = load(BED, j) + load(RIVER, j)
            for k in (EAST, NORTH, FLUX):
                self.state[k][at] = jnp.zeros((8, LANES), F32)

    def flows(self, pairs, drives):
        flood, _, q_east, q_north, _ = self.state
        for tiles in pairs:
            for t in tiles:
                for j in range(self.sizes[t]):
                    at = self.base[t] + j
                    self.sur[at] = self.g[at] + flood[at]
                    self.total[at] = jnp.zeros((8, LANES), F32)
        for tiles in pairs:
            for t in tiles:
                base, size = self.base[t], self.sizes[t]
                for j in range(size):
                    here = self.sur[base + j]
                    there = (
                        self.sur[base + j + 1] if j + 1 < size else pltpu.roll(self.sur[base], 7, 0)
                    )
                    q_east[base + j] = quotient(
                        q_east[base + j],
                        jnp.maximum(here, there) - self.e_base[base + j],
                        there - here,
                        self.e_fric[base + j],
                        DRIVE,
                    )
        for tiles in pairs:
            for j in range(self.sizes[tiles[0]]):
                surfaces = {t: self.sur[self.base[t] + j] for t in tiles}
                for t in tiles:
                    at = self.base[t] + j
                    there = self.northward(surfaces.get, t)
                    q_north[at] = quotient(
                        q_north[at],
                        jnp.maximum(surfaces[t], there) - self.n_base[at],
                        there - surfaces[t],
                        self.n_fric[at],
                        drives[t],
                    )

    def rivers(self):
        level, flux = self.state[LEVEL], self.state[FLUX]
        rate = SHORT_STEP * EXCHANGE

        def substep(_, carry):
            for t, size in enumerate(self.sizes):
                base = self.base[t]
                first = level[base]
                here = first
                first_flux = None
                last_flux = None
                for j in range(size):
                    at = base + j
                    there = level[at + 1] if j + 1 < size else pltpu.roll(first, 7, 0)
                    out = quotient(
                        flux[at],
                        jnp.maximum(here, there) - self.r_base[at],
                        there - here,
                        self.r_fric[at],
                        self.r_drive[at],
                    )
                    flux[at] = out
                    self.total[at] += here
                    if j:
                        level[at] = (
                            here
                            - rate * (here - self.sur[at])
                            + (last_flux - out) * self.r_inv[at]
                        )
                    else:
                        first_flux = out
                    last_flux = out
                    here = there
                level[base] = (
                    first
                    - rate * (first - self.sur[base])
                    + (pltpu.roll(last_flux, 1, 0) - first_flux) * self.r_inv[base]
                )
            return carry

        lax.fori_loop(0, SUB, substep, 0)

    def floods(self, pairs):
        flood, _, q_east, q_north, _ = self.state
        for tiles in pairs:
            for j in range(self.sizes[tiles[0]]):
                norths = {t: q_north[self.base[t] + j] for t in tiles}
                for t in tiles:
                    base, size = self.base[t], self.sizes[t]
                    at = base + j
                    west = q_east[at - 1] if j else pltpu.roll(q_east[base + size - 1], 1, 0)
                    flooded = flood[at] + (TIME_STEP / CELL_SIZE) * (
                        west - q_east[at] + self.southward(norths.get, t) - norths[t]
                    )
                    flood[at] = flooded + self.give[at] * (self.total[at] - SUB * self.sur[at])


def fold(low, high):
    lane = lax.broadcasted_iota(jnp.int32, (8, LANES), 1)
    return jnp.where(lane < 64, pltpu.roll(low, 16, 1), high)


def exchange_kernel(
    n_lon,
    n_lat,
    depth_hbm,
    ground_hbm,
    rough_hbm,
    river_hbm,
    width_hbm,
    bank_hbm,
    mask_hbm,
    ext,
    sides,
    strips,
    own_mask,
    inner,
    band,
    floats,
    ints,
    mask_in,
    top,
    bottom,
    load_sem,
    send_sem,
    recv_sem,
    *scratch,
):
    lon = lax.axis_index("lon")
    lat = lax.axis_index("lat")
    east = lax.rem(lon + 1, n_lon)
    west = lax.rem(lon + n_lon - 1, n_lon)
    north = lax.rem(lat + 1, n_lat)
    south = lax.rem(lat + n_lat - 1, n_lat)
    around = [
        (east, lat),
        (west, lat),
        (lon, north),
        (lon, south),
        (east, north),
        (west, north),
        (east, south),
        (west, south),
    ]
    around = [{"lon": a, "lat": b} for a, b in around]
    barrier = pltpu.get_barrier_semaphore()
    for device in around:
        pl.semaphore_signal(barrier, inc=1, device_id=device, device_id_type=MESH)

    loads = []
    for number, (source, target) in enumerate(
        [
            (ground_hbm, floats.at[GROUND]),
            (bank_hbm, ints.at[0]),
            (width_hbm, ints.at[1]),
            (river_hbm, floats.at[RIVER]),
            (depth_hbm, floats.at[DEPTH]),
            (rough_hbm, floats.at[ROUGH]),
            (mask_hbm, mask_in),
        ]
    ):
        copy = pltpu.make_async_copy(source, target, load_sem.at[number])
        copy.start()
        loads.append(copy)

    def place(field, values):
        for tile in range(2):
            ext[field, tile, HALO : HALO + COLS, :] = values[tile * LANES : (tile + 1) * LANES, :].T
        top[field] = values[0:8, :]
        bottom[field] = values[ROWS - 8 : ROWS, :]

    loads[0].wait()
    ground = floats[GROUND]
    place(GROUND, ground)
    loads[1].wait()
    place(BED, ground - (1.0 + 0.5 * ints[0].astype(F32)))
    loads[2].wait()
    place(WIDTH, 8.0 + 9.0 * ints[1].astype(F32))
    loads[3].wait()
    place(RIVER, floats[RIVER])
    loads[4].wait()
    place(DEPTH, floats[DEPTH])
    loads[5].wait()
    place(ROUGH, floats[ROUGH])
    loads[6].wait()
    for tile in range(2):
        own_mask[tile] = jnp.broadcast_to(mask_in[tile : tile + 1, :].astype(F32), (8, LANES))
    top[6] = own_mask[0]
    bottom[6] = own_mask[1]

    pl.semaphore_wait(barrier, len(around))
    fields = pl.ds(0, 6)
    both = pl.ds(0, 2)
    sends = [
        (
            ext.at[fields, both, pl.ds(COLS, HALO), :],
            ext.at[fields, both, pl.ds(0, HALO), :],
            around[0],
        ),
        (
            ext.at[fields, both, pl.ds(HALO, HALO), :],
            ext.at[fields, both, pl.ds(HALO + COLS, HALO), :],
            around[1],
        ),
        (bottom, strips.at[FROM_SW], around[4]),
        (bottom, strips.at[FROM_SE], around[5]),
        (top, strips.at[FROM_NW], around[6]),
        (top, strips.at[FROM_NE], around[7]),
        (bottom, strips.at[FROM_S], around[2]),
        (top, strips.at[FROM_N], around[3]),
        (own_mask, sides.at[0], around[0]),
        (own_mask, sides.at[1], around[1]),
    ]
    copies = []
    for number, (source, target, device) in enumerate(sends):
        copy = pltpu.make_async_remote_copy(
            src_ref=source,
            dst_ref=target,
            send_sem=send_sem.at[number],
            recv_sem=recv_sem.at[number],
            device_id=device,
            device_id_type=MESH,
        )
        copy.start()
        copies.append(copy)

    size = COLS // 8
    zone = Zone(scratch, [size, size], [1, 0])
    for tile in range(2):
        def load(field, j):
            return ext[field, tile, pl.ds(HALO + j, 8, stride=size), :]

        zone.prepare(tile, load, lambda c: c == COLS - 1, lambda c: own_mask[tile])
        zone.begin(tile, load)
    pairs = [(0, 1)]
    zone.prepare_north((0, 1))
    drives = [DRIVE, jnp.where((zone.lane == LANES - 1) & (lat == n_lat - 1), 0.0, DRIVE)]

    def step(number, carry):
        zone.flows(pairs, drives)
        zone.rivers()
        zone.floods(pairs)
        for k in range(STATE):
            for tile in range(2):
                for j in range(size):
                    inner[number, k, tile, pl.ds(j, 8, stride=size), :] = zone.state[k][
                        zone.base[tile] + j
                    ]
        return carry

    lax.fori_loop(0, STEPS, step, 0)

    for field in range(6):
        values = [
            fold(
                ext[field, 0, HALO + 8 * i : HALO + 8 * i + 8, :],
                ext[field, 1, HALO + 8 * i : HALO + 8 * i + 8, :],
            )
            for i in range(size)
        ]
        for i in range(BAND // 8):
            value = jnp.ones((8, LANES), F32)
            for k in range(4):
                at = 4 * k - 4 + i
                if 0 <= at < size:
                    moved = pltpu.roll(values[at], (32 * k + 8) % LANES, 1)
                    value = jnp.where(zone.lane // 32 == k, moved, value)
            band[field, 8 * i : 8 * i + 8, :] = value

    for copy in copies:
        copy.wait()


def flow_kernel(
    n_lat,
    ext,
    sides,
    strips,
    own_mask,
    inner,
    band,
    flood_out,
    river_out,
    east_out,
    north_out,
    rows,
    plain,
    ends,
    *scratch,
):
    lat = lax.axis_index("lat")
    size = STRIP // 8
    wide = BAND // 8
    zone = Zone(scratch, [size] * 4 + [wide], [1, 0, 3, 2, 4])
    lane, sublane = zone.lane, zone.sublane
    group, place = lane // 32, lane % 32
    halo_lane = (place >= 8) & (place < 24)
    row_tile = 4
    pairs = [(0, 1), (2, 3), (4,)]
    last_row = (lane == LANES - 1) & (lat == n_lat - 1)
    plain_drive = jnp.where(last_row, 0.0, DRIVE)
    row_closed = ((place == 7) & (lat == n_lat - 1)) | ((place == 23) & (lat == 0))
    drives = [DRIVE, plain_drive, DRIVE, plain_drive, jnp.where(row_closed, 0.0, DRIVE)]

    ones = jnp.ones((8, LANES), F32)
    for field in range(6):
        pieces = []
        for k in range(4):
            pieces.append(ones)
            for west, middle, east in (
                (FROM_NW, FROM_N, FROM_NE),
                (FROM_SW, FROM_S, FROM_SE),
            ):
                value = strips[middle, field]
                if k != 1:
                    value = pltpu.roll(value, (160 - 32 * k) % LANES, 1)
                if k == 0:
                    value = jnp.where(lane < 32, pltpu.roll(strips[west, field], 32, 1), value)
                if k == 3:
                    value = jnp.where(lane < 64, value, pltpu.roll(strips[east, field], 64, 1))
                pieces.append(value)
            pieces.append(ones)
        block = jnp.concatenate(pieces, axis=0).T
        for i in range(wide):
            value = band[field, 8 * i : 8 * i + 8, :]
            if 1 <= i < 4:
                at = 8 * (i - 1)
                moved = fold(ext[field, 0, at : at + 8, :], ext[field, 1, at : at + 8, :])
                value = jnp.where(group == 0, pltpu.roll(moved, 8, 1), value)
            if 8 <= i < 11:
                at = HALO + COLS + 8 * (i - 8)
                moved = fold(ext[field, 0, at : at + 8, :], ext[field, 1, at : at + 8, :])
                value = jnp.where(group == 3, pltpu.roll(moved, 104, 1), value)
            rows[field, 8 * i : 8 * i + 8, :] = jnp.where(
                halo_lane, block[8 * i : 8 * i + 8, :], value
            )

    def row_mask(low, high, north, south):
        value = jnp.where(place < 8, pltpu.roll(high, 8, 1), pltpu.roll(low, 24, 1))
        value = jnp.where(halo_lane & (place < 16), pltpu.roll(north, 8, 1), value)
        return jnp.where(halo_lane & (place >= 16), pltpu.roll(south, 24, 1), value)

    middle = row_mask(own_mask[0], own_mask[1], strips[FROM_N, 6], strips[FROM_S, 6])
    west = row_mask(sides[0, 0], sides[0, 1], strips[FROM_NW, 6], strips[FROM_SW, 6])
    east = row_mask(sides[1, 0], sides[1, 1], strips[FROM_NE, 6], strips[FROM_SE, 6])
    east = pltpu.roll(east, 96, 1)
    spread = middle
    for k in range(1, 4):
        spread = jnp.where(group == k, pltpu.roll(middle, 32 * k, 1), spread)

    def load_row(field, j):
        return rows[field, pl.ds(j, 8, stride=wide), :]

    zone.prepare(
        row_tile,
        load_row,
        lambda c: ((c == 31) & (group == 0)) | ((c == 63) & (group == 3)) | (c == BAND - 1),
        lambda c: jnp.where(
            (c < 32) & (group == 0), west, jnp.where((c >= 64) & (group == 3), east, spread)
        ),
    )
    zone.begin(row_tile, load_row)
    zone.prepare_north((row_tile,))

    def start_of(step, side):
        return STARTS[step] if side == 0 else WIDE - STRIP - STARTS[step]

    for step in range(STEPS):
        for side in range(2):
            start = start_of(step, side)
            for tile in range(2):
                t = 2 * side + tile

                def load(field, j):
                    return ext[field, tile, pl.ds(start + j, 8, stride=size), :]

                if step != 3:
                    zone.prepare(
                        t,
                        load,
                        lambda c: (c + start == HALO - 1)
                        | (c + start == HALO + COLS - 1)
                        | (c == STRIP - 1),
                        lambda c: jnp.where(
                            (c + start < HALO) if side == 0 else (c + start >= HALO + COLS),
                            sides[side, tile],
                            own_mask[tile],
                        ),
                    )
                if step == 0:
                    zone.begin(t, load)
                else:
                    for k in range(STATE):
                        if side == 0:
                            low, high = 8 * step, start + STRIP - HALO
                        else:
                            low, high = start - HALO, COLS - 8 * step
                        plain[k, tile, HALO + low : HALO + high, :] = inner[
                            step - 1, k, tile, low:high, :
                        ]
                        for j in range(size):
                            zone.state[k][zone.base[t] + j] = plain[
                                k, tile, pl.ds(start + j, 8, stride=size), :
                            ]
            if step != 3:
                zone.prepare_north((2 * side, 2 * side + 1))
        zone.flows(pairs, drives)
        zone.rivers()
        zone.floods(pairs)
        for side in range(2):
            start = start_of(step, side)
            for tile in range(2):
                t = 2 * side + tile
                for k in range(STATE):
                    for j in range(size):
                        plain[k, tile, pl.ds(start + j, 8, stride=size), :] = zone.state[k][
                            zone.base[t] + j
                        ]

    for k in range(4):
        for j in range(wide):
            ends[k, pl.ds(j, 8, stride=wide), :] = zone.state[k][zone.base[row_tile] + j]
    for k, target in enumerate((flood_out, river_out, east_out, north_out)):
        for tile in range(2):
            pieces = []
            for i in range(COLS // 8):
                if 3 <= i < 13:
                    value = inner[STEPS - 1, k, tile, 8 * i : 8 * i + 8, :]
                else:
                    value = plain[k, tile, HALO + 8 * i : HALO + 8 * i + 8, :]
                end = ends[k, 32 + 8 * (i % 4) : 40 + 8 * (i % 4), :]
                shift = 32 * (i // 4)
                if tile == 0:
                    value = jnp.where(lane < 4, pltpu.roll(end, (104 - shift) % LANES, 1), value)
                else:
                    value = jnp.where(lane < 124, value, pltpu.roll(end, (120 - shift) % LANES, 1))
                if k == LEVEL:
                    at = HALO + 8 * i
                    value = jnp.where(
                        own_mask[tile] > 0.0,
                        value - ext[BED, tile, at : at + 8, :],
                        ext[RIVER, tile, at : at + 8, :],
                    )
                pieces.append(value)
            target[tile * LANES : (tile + 1) * LANES, :] = jnp.concatenate(pieces, axis=0).T


def body(n_lon, n_lat, depth_init, ground, roughness, river_init, reach_mask, width_class, bank_class):
    mask = reach_mask.reshape(2, LANES)
    field = (ROWS, COLS)
    far = pl.BlockSpec(memory_space=pltpu.HBM)
    near = pl.BlockSpec(memory_space=pltpu.VMEM)
    state = [pltpu.VMEM((REGISTERS, 8, LANES), F32)] * SCRATCH
    handed = pl.pallas_call(
        functools.partial(exchange_kernel, n_lon, n_lat),
        out_shape=(
            pltpu.VMEM((6, 2, WIDE, LANES), F32),
            pltpu.VMEM((2, 2, 8, LANES), F32),
            pltpu.VMEM((6, 7, 8, LANES), F32),
            pltpu.VMEM((2, 8, LANES), F32),
            pltpu.VMEM((STEPS, STATE, 2, COLS, LANES), F32),
            pltpu.VMEM((6, BAND, LANES), F32),
        ),
        in_specs=[far] * 7,
        out_specs=(near,) * 6,
        scratch_shapes=[
            pltpu.VMEM((4, ROWS, COLS), F32),
            pltpu.VMEM((2, ROWS, COLS), jnp.int32),
            pltpu.VMEM((2, LANES), jnp.int32),
            pltpu.VMEM((7, 8, LANES), F32),
            pltpu.VMEM((7, 8, LANES), F32),
            pltpu.SemaphoreType.DMA((7,)),
            pltpu.SemaphoreType.DMA((10,)),
            pltpu.SemaphoreType.DMA((10,)),
        ]
        + state,
        compiler_params=pltpu.CompilerParams(
            collective_id=0, has_side_effects=True, vmem_limit_bytes=VMEM_LIMIT
        ),
        name="exchange",
    )(*[
        pltpu.with_memory_space_constraint(x, pltpu.HBM)
        for x in (depth_init, ground, roughness, river_init, width_class, bank_class, mask)
    ])
    handed = [pltpu.with_memory_space_constraint(x, pltpu.VMEM) for x in handed]
    return pl.pallas_call(
        functools.partial(flow_kernel, n_lat),
        out_shape=(jax.ShapeDtypeStruct(field, F32),) * 4,
        in_specs=[near] * 6,
        out_specs=(near,) * 4,
        scratch_shapes=[
            pltpu.VMEM((6, BAND, LANES), F32),
            pltpu.VMEM((STATE, 2, WIDE, LANES), F32),
            pltpu.VMEM((4, BAND, LANES), F32),
        ]
        + state,
        compiler_params=pltpu.CompilerParams(vmem_limit_bytes=VMEM_LIMIT),
        name="flow",
    )(*handed)


def solution(mesh):
    placed = P("lat", "lon")
    return jax.shard_map(
        functools.partial(body, mesh.shape["lon"], mesh.shape["lat"]),
        mesh=mesh,
        in_specs=(placed,) * 7,
        out_specs=(placed,) * 4,
        check_vma=False,
    )
```

```python
import functools
import math

import jax
import jax.numpy as jnp
from jax import lax
from jax.experimental import pallas as pl
from jax.experimental.pallas import tpu as pltpu
from jax.sharding import PartitionSpec as P

MESH = pl.DeviceIdType.MESH
F32 = jnp.float32
SUB = 8
STEPS = 4
ROWS = 256
COLS = 128
HALO = 24
WIDE = COLS + 2 * HALO
LANES = 128
STRIPS = (32, 32, 32, 40)
BAND = 96
STARTS = (0, 8, 16, 16)
DEPTH, GROUND, ROUGH, RIVER, WIDTH, BED = range(6)
FROM_S, FROM_N, FROM_SW, FROM_SE, FROM_NW, FROM_NE = range(6)
FLOOD, LEVEL, EAST, NORTH, FLUX = range(5)

GRAVITY = 9.81
CELL_SIZE = 90.0
TIME_STEP = 10.0
SHALLOW = 0.1
EXCHANGE = 0.01
CHANNEL_MANNING = 0.035
SHORT_STEP = TIME_STEP / SUB
POWER = -7.0 / 6.0 / math.log(2.0)
DRIVE = GRAVITY * TIME_STEP / CELL_SIZE

STATE = 5
SCRATCH = 17
REGISTERS = 32
VMEM_LIMIT = 24 << 20


def quotient(current, height, drop, friction, drive):
    power = jnp.exp2(POWER * jnp.log(height * height + SHALLOW * SHALLOW))
    resisted = 1.0 + friction * jnp.abs(current) * power
    return (current - drive * (height * drop)) / resisted


class Zone:
    def __init__(self, refs, sizes, partners):
        self.sizes = sizes
        self.partners = partners
        self.base = [sum(sizes[:t]) for t in range(len(sizes))]
        self.state = refs[:STATE]
        (
            self.g,
            self.sur,
            self.e_base,
            self.e_fric,
            self.n_base,
            self.n_fric,
            self.r_base,
            self.r_drive,
            self.r_fric,
            self.r_inv,
            self.give,
            self.total,
        ) = refs[STATE:]
        self.lane = lax.broadcasted_iota(jnp.int32, (8, LANES), 1)
        self.sublane = lax.broadcasted_iota(jnp.int32, (8, LANES), 0)

    def column(self, tile, j):
        return self.sublane * self.sizes[tile] + j

    def northward(self, read, tile):
        here = pltpu.roll(read(tile), LANES - 1, 1)
        if self.partners[tile] == tile:
            return here
        there = pltpu.roll(read(self.partners[tile]), LANES - 1, 1)
        return jnp.where(self.lane == LANES - 1, there, here)

    def southward(self, read, tile):
        here = pltpu.roll(read(tile), 1, 1)
        if self.partners[tile] == tile:
            return here
        there = pltpu.roll(read(self.partners[tile]), 1, 1)
        return jnp.where(self.lane == 0, there, here)

    def prepare(self, tile, load, closed, mask):
        size, base = self.sizes[tile], self.base[tile]

        def after(values, j):
            return values[j + 1] if j + 1 < size else pltpu.roll(values[0], 7, 0)

        grounds = [load(GROUND, j) for j in range(size)]
        roughs = [load(ROUGH, j) for j in range(size)]
        beds = [load(BED, j) for j in range(size)]
        widths = [load(WIDTH, j) for j in range(size)]
        for j in range(size):
            at = base + j
            column = self.column(tile, j)
            self.g[at] = grounds[j]
            self.e_base[at] = jnp.maximum(grounds[j], after(grounds, j))
            self.e_fric[at] = (GRAVITY * TIME_STEP) * (roughs[j] * after(roughs, j))
            self.n_fric[at] = roughs[j]
            breadth = 0.5 * (widths[j] + after(widths, j))
            self.r_base[at] = jnp.maximum(beds[j], after(beds, j))
            self.r_drive[at] = jnp.where(
                closed(column), 0.0, (GRAVITY * SHORT_STEP / CELL_SIZE) * breadth
            )
            self.r_fric[at] = (
                GRAVITY * SHORT_STEP * CHANNEL_MANNING * CHANNEL_MANNING
            ) / breadth
            self.r_inv[at] = SHORT_STEP / (CELL_SIZE * widths[j])
            self.give[at] = mask(column) * widths[j] * (SHORT_STEP * EXCHANGE / CELL_SIZE)

    def prepare_north(self, tiles):
        for j in range(self.sizes[tiles[0]]):
            grounds = {t: self.g[self.base[t] + j] for t in tiles}
            roughs = {t: self.n_fric[self.base[t] + j] for t in tiles}
            for t in tiles:
                at = self.base[t] + j
                self.n_base[at] = jnp.maximum(grounds[t], self.northward(grounds.get, t))
                self.n_fric[at] = (GRAVITY * TIME_STEP) * (
                    roughs[t] * self.northward(roughs.get, t)
                )

    def begin(self, tile, load):
        for j in range(self.sizes[tile]):
            at = self.base[tile] + j
            self.state[FLOOD][at] = load(DEPTH, j)
            self.state[LEVEL][at] = load(BED, j) + load(RIVER, j)
            for k in (EAST, NORTH, FLUX):
                self.state[k][at] = jnp.zeros((8, LANES), F32)

    def flows(self, pairs, drives):
        flood, _, q_east, q_north, _ = self.state
        for tiles in pairs:
            for t in tiles:
                for j in range(self.sizes[t]):
                    at = self.base[t] + j
                    self.sur[at] = self.g[at] + flood[at]
                    self.total[at] = jnp.zeros((8, LANES), F32)
        for tiles in pairs:
            for t in tiles:
                base, size = self.base[t], self.sizes[t]
                for j in range(size):
                    here = self.sur[base + j]
                    there = (
                        self.sur[base + j + 1] if j + 1 < size else pltpu.roll(self.sur[base], 7, 0)
                    )
                    q_east[base + j] = quotient(
                        q_east[base + j],
                        jnp.maximum(here, there) - self.e_base[base + j],
                        there - here,
                        self.e_fric[base + j],
                        DRIVE,
                    )
        for tiles in pairs:
            for j in range(self.sizes[tiles[0]]):
                surfaces = {t: self.sur[self.base[t] + j] for t in tiles}
                for t in tiles:
                    at = self.base[t] + j
                    there = self.northward(surfaces.get, t)
                    q_north[at] = quotient(
                        q_north[at],
                        jnp.maximum(surfaces[t], there) - self.n_base[at],
                        there - surfaces[t],
                        self.n_fric[at],
                        drives[t],
                    )

    def rivers(self):
        level, flux = self.state[LEVEL], self.state[FLUX]
        rate = SHORT_STEP * EXCHANGE

        def substep(_, carry):
            for t, size in enumerate(self.sizes):
                base = self.base[t]
                first = level[base]
                here = first
                first_flux = None
                last_flux = None
                for j in range(size):
                    at = base + j
                    there = level[at + 1] if j + 1 < size else pltpu.roll(first, 7, 0)
                    out = quotient(
                        flux[at],
                        jnp.maximum(here, there) - self.r_base[at],
                        there - here,
                        self.r_fric[at],
                        self.r_drive[at],
                    )
                    flux[at] = out
                    self.total[at] += here
                    if j:
                        level[at] = (
                            here
                            - rate * (here - self.sur[at])
                            + (last_flux - out) * self.r_inv[at]
                        )
                    else:
                        first_flux = out
                    last_flux = out
                    here = there
                level[base] = (
                    first
                    - rate * (first - self.sur[base])
                    + (pltpu.roll(last_flux, 1, 0) - first_flux) * self.r_inv[base]
                )
            return carry

        lax.fori_loop(0, SUB, substep, 0)

    def floods(self, pairs):
        flood, _, q_east, q_north, _ = self.state
        for tiles in pairs:
            for j in range(self.sizes[tiles[0]]):
                norths = {t: q_north[self.base[t] + j] for t in tiles}
                for t in tiles:
                    base, size = self.base[t], self.sizes[t]
                    at = base + j
                    west = q_east[at - 1] if j else pltpu.roll(q_east[base + size - 1], 1, 0)
                    flooded = flood[at] + (TIME_STEP / CELL_SIZE) * (
                        west - q_east[at] + self.southward(norths.get, t) - norths[t]
                    )
                    flood[at] = flooded + self.give[at] * (self.total[at] - SUB * self.sur[at])


def fold(low, high):
    lane = lax.broadcasted_iota(jnp.int32, (8, LANES), 1)
    return jnp.where(lane < 64, pltpu.roll(low, 16, 1), high)


def exchange_kernel(
    n_lon,
    n_lat,
    depth_hbm,
    ground_hbm,
    rough_hbm,
    river_hbm,
    width_hbm,
    bank_hbm,
    mask_hbm,
    ext,
    sides,
    strips,
    own_mask,
    inner,
    band,
    plain,
    floats,
    ints,
    mask_in,
    top,
    bottom,
    load_sem,
    send_sem,
    recv_sem,
    *scratch,
):
    lon = lax.axis_index("lon")
    lat = lax.axis_index("lat")
    east = lax.rem(lon + 1, n_lon)
    west = lax.rem(lon + n_lon - 1, n_lon)
    north = lax.rem(lat + 1, n_lat)
    south = lax.rem(lat + n_lat - 1, n_lat)
    around = [
        (east, lat),
        (west, lat),
        (lon, north),
        (lon, south),
        (east, north),
        (west, north),
        (east, south),
        (west, south),
    ]
    around = [{"lon": a, "lat": b} for a, b in around]
    barrier = pltpu.get_barrier_semaphore()
    for device in around:
        pl.semaphore_signal(barrier, inc=1, device_id=device, device_id_type=MESH)

    loads = []
    for number, (source, target) in enumerate(
        [
            (ground_hbm, floats.at[GROUND]),
            (bank_hbm, ints.at[0]),
            (width_hbm, ints.at[1]),
            (river_hbm, floats.at[RIVER]),
            (depth_hbm, floats.at[DEPTH]),
            (rough_hbm, floats.at[ROUGH]),
            (mask_hbm, mask_in),
        ]
    ):
        copy = pltpu.make_async_copy(source, target, load_sem.at[number])
        copy.start()
        loads.append(copy)

    def place(field, values):
        for tile in range(2):
            ext[field, tile, HALO : HALO + COLS, :] = values[tile * LANES : (tile + 1) * LANES, :].T
        top[field] = values[0:8, :]
        bottom[field] = values[ROWS - 8 : ROWS, :]

    loads[0].wait()
    ground = floats[GROUND]
    place(GROUND, ground)
    loads[1].wait()
    place(BED, ground - (1.0 + 0.5 * ints[0].astype(F32)))
    loads[2].wait()
    place(WIDTH, 8.0 + 9.0 * ints[1].astype(F32))
    loads[3].wait()
    place(RIVER, floats[RIVER])
    loads[4].wait()
    place(DEPTH, floats[DEPTH])
    loads[5].wait()
    place(ROUGH, floats[ROUGH])
    loads[6].wait()
    for tile in range(2):
        own_mask[tile] = jnp.broadcast_to(mask_in[tile : tile + 1, :].astype(F32), (8, LANES))
    top[6] = own_mask[0]
    bottom[6] = own_mask[1]

    pl.semaphore_wait(barrier, len(around))
    fields = pl.ds(0, 6)
    both = pl.ds(0, 2)
    sends = [
        (
            ext.at[fields, both, pl.ds(COLS, HALO), :],
            ext.at[fields, both, pl.ds(0, HALO), :],
            around[0],
        ),
        (
            ext.at[fields, both, pl.ds(HALO, HALO), :],
            ext.at[fields, both, pl.ds(HALO + COLS, HALO), :],
            around[1],
        ),
        (bottom, strips.at[FROM_SW], around[4]),
        (bottom, strips.at[FROM_SE], around[5]),
        (top, strips.at[FROM_NW], around[6]),
        (top, strips.at[FROM_NE], around[7]),
        (bottom, strips.at[FROM_S], around[2]),
        (top, strips.at[FROM_N], around[3]),
        (own_mask, sides.at[0], around[0]),
        (own_mask, sides.at[1], around[1]),
    ]
    copies = []
    for number, (source, target, device) in enumerate(sends):
        copy = pltpu.make_async_remote_copy(
            src_ref=source,
            dst_ref=target,
            send_sem=send_sem.at[number],
            recv_sem=recv_sem.at[number],
            device_id=device,
            device_id_type=MESH,
        )
        copy.start()
        copies.append(copy)

    size = COLS // 8
    zone = Zone(scratch, [size, size], [1, 0])
    for tile in range(2):
        def load(field, j):
            return ext[field, tile, pl.ds(HALO + j, 8, stride=size), :]

        zone.prepare(tile, load, lambda c: c == COLS - 1, lambda c: own_mask[tile])
        zone.begin(tile, load)
    pairs = [(0, 1)]
    zone.prepare_north((0, 1))
    drives = [DRIVE, jnp.where((zone.lane == LANES - 1) & (lat == n_lat - 1), 0.0, DRIVE)]

    def step(number, carry):
        zone.flows(pairs, drives)
        zone.rivers()
        zone.floods(pairs)
        for k in range(STATE):
            for tile in range(2):
                for j in range(size):
                    inner[number, k, tile, pl.ds(j, 8, stride=size), :] = zone.state[k][
                        zone.base[tile] + j
                    ]
        return carry

    lax.fori_loop(0, STEPS, step, 0)

    for field in range(6):
        values = [
            fold(
                ext[field, 0, HALO + 8 * i : HALO + 8 * i + 8, :],
                ext[field, 1, HALO + 8 * i : HALO + 8 * i + 8, :],
            )
            for i in range(size)
        ]
        for i in range(BAND // 8):
            value = jnp.ones((8, LANES), F32)
            for k in range(4):
                at = 4 * k - 4 + i
                if 0 <= at < size:
                    moved = pltpu.roll(values[at], (32 * k + 8) % LANES, 1)
                    value = jnp.where(zone.lane // 32 == k, moved, value)
            band[field, 8 * i : 8 * i + 8, :] = value

    side_copies = (0, 1, 8, 9)
    for number in side_copies:
        copies[number].wait()
    for step in range(STEPS):
        strip = STRIPS[step]
        size = strip // 8
        zone = Zone(scratch, [size] * 4, [1, 0, 3, 2])
        pairs = [(0, 1), (2, 3)]
        for side in range(2):
            start = start_of(step, side)
            for tile in range(2):
                t = 2 * side + tile

                def load(field, j):
                    return ext[field, tile, pl.ds(start + j, 8, stride=size), :]

                zone.prepare(
                    t,
                    load,
                    lambda c: (c + start == HALO - 1)
                    | (c + start == HALO + COLS - 1)
                    | (c == strip - 1),
                    lambda c: jnp.where(
                        (c + start < HALO) if side == 0 else (c + start >= HALO + COLS),
                        sides[side, tile],
                        own_mask[tile],
                    ),
                )
                if step == 0:
                    zone.begin(t, load)
                    continue
                for k in range(STATE):
                    if side == 0:
                        low, high = 8 * (step - 1), start + strip - HALO
                        edge, kept = low, zone.sublane == 0
                    else:
                        low, high = start - HALO, COLS - 8 * (step - 1)
                        edge, kept = high - 8, zone.sublane == 7
                    for at in range(low, high, 8):
                        value = inner[step - 1, k, tile, at : at + 8, :]
                        if step == 1 and at == edge and k in (FLOOD, EAST):
                            old = plain[k, tile, HALO + at : HALO + at + 8, :]
                            value = jnp.where(kept, old, value)
                        plain[k, tile, HALO + at : HALO + at + 8, :] = value
                    for j in range(size):
                        zone.state[k][zone.base[t] + j] = plain[
                            k, tile, pl.ds(start + j, 8, stride=size), :
                        ]
            zone.prepare_north((2 * side, 2 * side + 1))
        zone.flows(pairs, [drives[0], drives[1], drives[0], drives[1]])
        zone.rivers()
        zone.floods(pairs)
        for side in range(2):
            start = start_of(step, side)
            for tile in range(2):
                t = 2 * side + tile
                for k in range(STATE if step < STEPS - 1 else 4):
                    for j in range(size):
                        plain[k, tile, pl.ds(start + j, 8, stride=size), :] = zone.state[k][
                            zone.base[t] + j
                        ]
    for number, copy in enumerate(copies):
        if number not in side_copies:
            copy.wait()


def start_of(step, side):
    return STARTS[step] if side == 0 else WIDE - STRIPS[step] - STARTS[step]


def flow_kernel(
    n_lat,
    ext,
    sides,
    strips,
    own_mask,
    inner,
    band,
    plain,
    flood_out,
    river_out,
    east_out,
    north_out,
    rows,
    ends,
    stage,
    sems,
    *scratch,
):
    lat = lax.axis_index("lat")
    wide = BAND // 8
    zone = Zone(scratch, [wide], [0])
    lane, sublane = zone.lane, zone.sublane
    group, place = lane // 32, lane % 32
    halo_lane = (place >= 8) & (place < 24)
    pairs = [(0,)]
    row_closed = ((place == 7) & (lat == n_lat - 1)) | ((place == 23) & (lat == 0))
    drives = [jnp.where(row_closed, 0.0, DRIVE)]
    outs = (flood_out, river_out, east_out, north_out)

    copies = []
    for k in (EAST, NORTH, FLOOD, LEVEL):
        for tile in range(2):
            pieces = []
            for i in range(COLS // 8):
                if 3 <= i < 13:
                    value = inner[STEPS - 1, k, tile, 8 * i : 8 * i + 8, :]
                else:
                    value = plain[k, tile, HALO + 8 * i : HALO + 8 * i + 8, :]
                if k == LEVEL:
                    at = HALO + 8 * i
                    value = jnp.where(
                        own_mask[tile] > 0.0,
                        value - ext[BED, tile, at : at + 8, :],
                        ext[RIVER, tile, at : at + 8, :],
                    )
                pieces.append(value)
            stage[k, tile * LANES : (tile + 1) * LANES, :] = jnp.concatenate(pieces, axis=0).T
        body_rows = pl.ds(8, ROWS - 16)
        copy = pltpu.make_async_copy(stage.at[k, body_rows], outs[k].at[body_rows], sems.at[k])
        copy.start()
        copies.append(copy)

    ones = jnp.ones((8, LANES), F32)
    for field in range(6):
        pieces = []
        for k in range(4):
            pieces.append(ones)
            for west, middle, east in (
                (FROM_NW, FROM_N, FROM_NE),
                (FROM_SW, FROM_S, FROM_SE),
            ):
                value = strips[middle, field]
                if k != 1:
                    value = pltpu.roll(value, (160 - 32 * k) % LANES, 1)
                if k == 0:
                    value = jnp.where(lane < 32, pltpu.roll(strips[west, field], 32, 1), value)
                if k == 3:
                    value = jnp.where(lane < 64, value, pltpu.roll(strips[east, field], 64, 1))
                pieces.append(value)
            pieces.append(ones)
        block = jnp.concatenate(pieces, axis=0).T
        for i in range(wide):
            value = band[field, 8 * i : 8 * i + 8, :]
            if 1 <= i < 4:
                at = 8 * (i - 1)
                moved = fold(ext[field, 0, at : at + 8, :], ext[field, 1, at : at + 8, :])
                value = jnp.where(group == 0, pltpu.roll(moved, 8, 1), value)
            if 8 <= i < 11:
                at = HALO + COLS + 8 * (i - 8)
                moved = fold(ext[field, 0, at : at + 8, :], ext[field, 1, at : at + 8, :])
                value = jnp.where(group == 3, pltpu.roll(moved, 104, 1), value)
            rows[field, 8 * i : 8 * i + 8, :] = jnp.where(
                halo_lane, block[8 * i : 8 * i + 8, :], value
            )

    def row_mask(low, high, north, south):
        value = jnp.where(place < 8, pltpu.roll(high, 8, 1), pltpu.roll(low, 24, 1))
        value = jnp.where(halo_lane & (place < 16), pltpu.roll(north, 8, 1), value)
        return jnp.where(halo_lane & (place >= 16), pltpu.roll(south, 24, 1), value)

    middle = row_mask(own_mask[0], own_mask[1], strips[FROM_N, 6], strips[FROM_S, 6])
    west = row_mask(sides[0, 0], sides[0, 1], strips[FROM_NW, 6], strips[FROM_SW, 6])
    east = row_mask(sides[1, 0], sides[1, 1], strips[FROM_NE, 6], strips[FROM_SE, 6])
    east = pltpu.roll(east, 96, 1)
    spread = middle
    for k in range(1, 4):
        spread = jnp.where(group == k, pltpu.roll(middle, 32 * k, 1), spread)

    def load_row(field, j):
        return rows[field, pl.ds(j, 8, stride=wide), :]

    zone.prepare(
        0,
        load_row,
        lambda c: ((c == 31) & (group == 0)) | ((c == 63) & (group == 3)) | (c == BAND - 1),
        lambda c: jnp.where(
            (c < 32) & (group == 0), west, jnp.where((c >= 64) & (group == 3), east, spread)
        ),
    )
    zone.begin(0, load_row)
    zone.prepare_north((0,))

    for _ in range(STEPS):
        zone.flows(pairs, drives)
        zone.rivers()
        zone.floods(pairs)

    for k in range(4):
        for j in range(wide):
            ends[k, pl.ds(j, 8, stride=wide), :] = zone.state[k][zone.base[0] + j]
    pieces = []
    for k in range(4):
        for at in range(32, 64, 8):
            value = ends[k, at : at + 8, :]
            if k == LEVEL:
                value = jnp.where(
                    spread > 0.0,
                    value - rows[BED, at : at + 8, :],
                    rows[RIVER, at : at + 8, :],
                )
            pieces.append(value)
    turned = jnp.concatenate(pieces, axis=0).T
    for k in range(4):
        for which in range(2):
            value = None
            for g in range(4):
                at = 32 * g + (24 if which == 0 else 0)
                piece = turned[at : at + 8, :]
                shift = (32 * g - 32 * k) % LANES
                piece = pltpu.roll(piece, shift, 1) if shift else piece
                value = piece if value is None else jnp.where(group == g, piece, value)
            first = 0 if which == 0 else ROWS - 8
            taken = (sublane < 4) if which == 0 else (sublane >= 4)
            end_rows = pl.ds(first, 8)
            stage[k, end_rows, :] = jnp.where(taken, value, stage[k, end_rows, :])
            copy = pltpu.make_async_copy(
                stage.at[k, end_rows], outs[k].at[end_rows], sems.at[4 + 2 * k + which]
            )
            copy.start()
            copies.append(copy)
    for copy in copies:
        copy.wait()


def body(n_lon, n_lat, depth_init, ground, roughness, river_init, reach_mask, width_class, bank_class):
    mask = reach_mask.reshape(2, LANES)
    field = (ROWS, COLS)
    far = pl.BlockSpec(memory_space=pltpu.HBM)
    near = pl.BlockSpec(memory_space=pltpu.VMEM)
    state = [pltpu.VMEM((REGISTERS, 8, LANES), F32)] * SCRATCH
    handed = pl.pallas_call(
        functools.partial(exchange_kernel, n_lon, n_lat),
        out_shape=(
            pltpu.VMEM((6, 2, WIDE, LANES), F32),
            pltpu.VMEM((2, 2, 8, LANES), F32),
            pltpu.VMEM((6, 7, 8, LANES), F32),
            pltpu.VMEM((2, 8, LANES), F32),
            pltpu.VMEM((STEPS, STATE, 2, COLS, LANES), F32),
            pltpu.VMEM((6, BAND, LANES), F32),
            pltpu.VMEM((STATE, 2, WIDE, LANES), F32),
        ),
        in_specs=[far] * 7,
        out_specs=(near,) * 7,
        scratch_shapes=[
            pltpu.VMEM((4, ROWS, COLS), F32),
            pltpu.VMEM((2, ROWS, COLS), jnp.int32),
            pltpu.VMEM((2, LANES), jnp.int32),
            pltpu.VMEM((7, 8, LANES), F32),
            pltpu.VMEM((7, 8, LANES), F32),
            pltpu.SemaphoreType.DMA((7,)),
            pltpu.SemaphoreType.DMA((10,)),
            pltpu.SemaphoreType.DMA((10,)),
        ]
        + state,
        compiler_params=pltpu.CompilerParams(
            collective_id=0, has_side_effects=True, vmem_limit_bytes=VMEM_LIMIT
        ),
        name="exchange",
    )(*[
        pltpu.with_memory_space_constraint(x, pltpu.HBM)
        for x in (depth_init, ground, roughness, river_init, width_class, bank_class, mask)
    ])
    handed = [pltpu.with_memory_space_constraint(x, pltpu.VMEM) for x in handed]
    return pl.pallas_call(
        functools.partial(flow_kernel, n_lat),
        out_shape=(jax.ShapeDtypeStruct(field, F32),) * 4,
        in_specs=[near] * 7,
        out_specs=(far,) * 4,
        scratch_shapes=[
            pltpu.VMEM((6, BAND, LANES), F32),
            pltpu.VMEM((4, BAND, LANES), F32),
            pltpu.VMEM((4, ROWS, COLS), F32),
            pltpu.SemaphoreType.DMA((12,)),
        ]
        + state,
        compiler_params=pltpu.CompilerParams(vmem_limit_bytes=VMEM_LIMIT),
        name="flow",
    )(*handed)


def solution(mesh):
    placed = P("lat", "lon")
    return jax.shard_map(
        functools.partial(body, mesh.shape["lon"], mesh.shape["lat"]),
        mesh=mesh,
        in_specs=(placed,) * 7,
        out_specs=(placed,) * 4,
        check_vma=False,
    )
```

```python
import functools
import math

import jax
import jax.numpy as jnp
from jax import lax
from jax.experimental import pallas as pl
from jax.experimental.pallas import tpu as pltpu
from jax.sharding import PartitionSpec as P

MESH = pl.DeviceIdType.MESH
F32 = jnp.float32
SUB = 8
STEPS = 4
ROWS = 256
COLS = 128
HALO = 24
WIDE = COLS + 2 * HALO
LANES = 128
STRIPS = (32, 40)
BAND = 96
DEPTH, GROUND, ROUGH, RIVER, WIDTH, BED = range(6)
FROM_S, FROM_N = range(2)
FLOOD, LEVEL, EAST, NORTH, FLUX = range(5)

GRAVITY = 9.81
CELL_SIZE = 90.0
TIME_STEP = 10.0
SHALLOW = 0.1
EXCHANGE = 0.01
CHANNEL_MANNING = 0.035
SHORT_STEP = TIME_STEP / SUB
POWER = -7.0 / 6.0 / math.log(2.0)
DRIVE = GRAVITY * TIME_STEP / CELL_SIZE

STATE = 5
SCRATCH = 17
REGISTERS = 32
VMEM_LIMIT = 24 << 20


def quotient(current, height, drop, friction, drive):
    power = jnp.exp2(POWER * jnp.log(height * height + SHALLOW * SHALLOW))
    resisted = 1.0 + friction * jnp.abs(current) * power
    return (current - drive * (height * drop)) / resisted


class Zone:
    def __init__(self, refs, sizes, partners):
        self.sizes = sizes
        self.partners = partners
        self.base = [sum(sizes[:t]) for t in range(len(sizes))]
        self.state = refs[:STATE]
        (
            self.g,
            self.sur,
            self.e_base,
            self.e_fric,
            self.n_base,
            self.n_fric,
            self.r_base,
            self.r_drive,
            self.r_fric,
            self.r_inv,
            self.give,
            self.total,
        ) = refs[STATE:]
        self.lane = lax.broadcasted_iota(jnp.int32, (8, LANES), 1)
        self.sublane = lax.broadcasted_iota(jnp.int32, (8, LANES), 0)

    def column(self, tile, j):
        return self.sublane * self.sizes[tile] + j

    def northward(self, read, tile):
        here = pltpu.roll(read(tile), LANES - 1, 1)
        if self.partners[tile] == tile:
            return here
        there = pltpu.roll(read(self.partners[tile]), LANES - 1, 1)
        return jnp.where(self.lane == LANES - 1, there, here)

    def southward(self, read, tile):
        here = pltpu.roll(read(tile), 1, 1)
        if self.partners[tile] == tile:
            return here
        there = pltpu.roll(read(self.partners[tile]), 1, 1)
        return jnp.where(self.lane == 0, there, here)

    def prepare(self, tile, load, closed, mask):
        size, base = self.sizes[tile], self.base[tile]

        def after(values, j):
            return values[j + 1] if j + 1 < size else pltpu.roll(values[0], 7, 0)

        grounds = [load(GROUND, j) for j in range(size)]
        roughs = [load(ROUGH, j) for j in range(size)]
        beds = [load(BED, j) for j in range(size)]
        widths = [load(WIDTH, j) for j in range(size)]
        for j in range(size):
            at = base + j
            column = self.column(tile, j)
            self.g[at] = grounds[j]
            self.e_base[at] = jnp.maximum(grounds[j], after(grounds, j))
            self.e_fric[at] = (GRAVITY * TIME_STEP) * (roughs[j] * after(roughs, j))
            self.n_fric[at] = roughs[j]
            breadth = 0.5 * (widths[j] + after(widths, j))
            self.r_base[at] = jnp.maximum(beds[j], after(beds, j))
            self.r_drive[at] = jnp.where(
                closed(column), 0.0, (GRAVITY * SHORT_STEP / CELL_SIZE) * breadth
            )
            self.r_fric[at] = (
                GRAVITY * SHORT_STEP * CHANNEL_MANNING * CHANNEL_MANNING
            ) / breadth
            self.r_inv[at] = SHORT_STEP / (CELL_SIZE * widths[j])
            self.give[at] = mask(column) * widths[j] * (SHORT_STEP * EXCHANGE / CELL_SIZE)

    def prepare_north(self, tiles):
        for j in range(self.sizes[tiles[0]]):
            grounds = {t: self.g[self.base[t] + j] for t in tiles}
            roughs = {t: self.n_fric[self.base[t] + j] for t in tiles}
            for t in tiles:
                at = self.base[t] + j
                self.n_base[at] = jnp.maximum(grounds[t], self.northward(grounds.get, t))
                self.n_fric[at] = (GRAVITY * TIME_STEP) * (
                    roughs[t] * self.northward(roughs.get, t)
                )

    def begin(self, tile, load):
        for j in range(self.sizes[tile]):
            at = self.base[tile] + j
            self.state[FLOOD][at] = load(DEPTH, j)
            self.state[LEVEL][at] = load(BED, j) + load(RIVER, j)
            for k in (EAST, NORTH, FLUX):
                self.state[k][at] = jnp.zeros((8, LANES), F32)

    def flows(self, pairs, drives):
        flood, _, q_east, q_north, _ = self.state
        for tiles in pairs:
            for t in tiles:
                for j in range(self.sizes[t]):
                    at = self.base[t] + j
                    self.sur[at] = self.g[at] + flood[at]
                    self.total[at] = jnp.zeros((8, LANES), F32)
        for tiles in pairs:
            for t in tiles:
                base, size = self.base[t], self.sizes[t]
                for j in range(size):
                    here = self.sur[base + j]
                    there = (
                        self.sur[base + j + 1] if j + 1 < size else pltpu.roll(self.sur[base], 7, 0)
                    )
                    q_east[base + j] = quotient(
                        q_east[base + j],
                        jnp.maximum(here, there) - self.e_base[base + j],
                        there - here,
                        self.e_fric[base + j],
                        DRIVE,
                    )
        for tiles in pairs:
            for j in range(self.sizes[tiles[0]]):
                surfaces = {t: self.sur[self.base[t] + j] for t in tiles}
                for t in tiles:
                    at = self.base[t] + j
                    there = self.northward(surfaces.get, t)
                    q_north[at] = quotient(
                        q_north[at],
                        jnp.maximum(surfaces[t], there) - self.n_base[at],
                        there - surfaces[t],
                        self.n_fric[at],
                        drives[t],
                    )

    def rivers(self):
        level, flux = self.state[LEVEL], self.state[FLUX]
        rate = SHORT_STEP * EXCHANGE

        def substep(_, carry):
            for t, size in enumerate(self.sizes):
                base = self.base[t]
                first = level[base]
                here = first
                first_flux = None
                last_flux = None
                for j in range(size):
                    at = base + j
                    there = level[at + 1] if j + 1 < size else pltpu.roll(first, 7, 0)
                    out = quotient(
                        flux[at],
                        jnp.maximum(here, there) - self.r_base[at],
                        there - here,
                        self.r_fric[at],
                        self.r_drive[at],
                    )
                    flux[at] = out
                    self.total[at] += here
                    if j:
                        level[at] = (
                            here
                            - rate * (here - self.sur[at])
                            + (last_flux - out) * self.r_inv[at]
                        )
                    else:
                        first_flux = out
                    last_flux = out
                    here = there
                level[base] = (
                    first
                    - rate * (first - self.sur[base])
                    + (pltpu.roll(last_flux, 1, 0) - first_flux) * self.r_inv[base]
                )
            return carry

        lax.fori_loop(0, SUB, substep, 0)

    def floods(self, pairs):
        flood, _, q_east, q_north, _ = self.state
        for tiles in pairs:
            for j in range(self.sizes[tiles[0]]):
                norths = {t: q_north[self.base[t] + j] for t in tiles}
                for t in tiles:
                    base, size = self.base[t], self.sizes[t]
                    at = base + j
                    west = q_east[at - 1] if j else pltpu.roll(q_east[base + size - 1], 1, 0)
                    flooded = flood[at] + (TIME_STEP / CELL_SIZE) * (
                        west - q_east[at] + self.southward(norths.get, t) - norths[t]
                    )
                    flood[at] = flooded + self.give[at] * (self.total[at] - SUB * self.sur[at])


def fold(low, high):
    lane = lax.broadcasted_iota(jnp.int32, (8, LANES), 1)
    return jnp.where(lane < 64, pltpu.roll(low, 16, 1), high)


def exchange_kernel(
    n_lon,
    n_lat,
    depth_hbm,
    ground_hbm,
    rough_hbm,
    river_hbm,
    width_hbm,
    bank_hbm,
    mask_hbm,
    ext,
    sides,
    strips,
    corners,
    own_mask,
    inner,
    band,
    plain,
    floats,
    ints,
    mask_in,
    top,
    bottom,
    packed,
    load_sem,
    send_sem,
    recv_sem,
    *scratch,
):
    lon = lax.axis_index("lon")
    lat = lax.axis_index("lat")
    east = lax.rem(lon + 1, n_lon)
    west = lax.rem(lon + n_lon - 1, n_lon)
    north = lax.rem(lat + 1, n_lat)
    south = lax.rem(lat + n_lat - 1, n_lat)
    around = [
        (east, lat),
        (west, lat),
        (lon, north),
        (lon, south),
    ]
    around = [{"lon": a, "lat": b} for a, b in around]
    barrier = pltpu.get_barrier_semaphore()
    for device in around:
        pl.semaphore_signal(barrier, inc=1, device_id=device, device_id_type=MESH)

    loads = []
    for number, (source, target) in enumerate(
        [
            (ground_hbm, floats.at[GROUND]),
            (bank_hbm, ints.at[0]),
            (width_hbm, ints.at[1]),
            (river_hbm, floats.at[RIVER]),
            (depth_hbm, floats.at[DEPTH]),
            (rough_hbm, floats.at[ROUGH]),
            (mask_hbm, mask_in),
        ]
    ):
        copy = pltpu.make_async_copy(source, target, load_sem.at[number])
        copy.start()
        loads.append(copy)

    def place(field, values):
        for tile in range(2):
            ext[field, tile, HALO : HALO + COLS, :] = values[tile * LANES : (tile + 1) * LANES, :].T
        top[field] = values[0:8, :]
        bottom[field] = values[ROWS - 8 : ROWS, :]

    loads[0].wait()
    ground = floats[GROUND]
    place(GROUND, ground)
    loads[1].wait()
    place(BED, ground - (1.0 + 0.5 * ints[0].astype(F32)))
    loads[2].wait()
    place(WIDTH, 8.0 + 9.0 * ints[1].astype(F32))
    loads[3].wait()
    place(RIVER, floats[RIVER])
    loads[4].wait()
    place(DEPTH, floats[DEPTH])
    loads[5].wait()
    place(ROUGH, floats[ROUGH])
    loads[6].wait()
    for tile in range(2):
        own_mask[tile] = jnp.broadcast_to(mask_in[tile : tile + 1, :].astype(F32), (8, LANES))
    top[6] = own_mask[0]
    bottom[6] = own_mask[1]

    pl.semaphore_wait(barrier, len(around))
    fields = pl.ds(0, 6)
    both = pl.ds(0, 2)
    sends = [
        (
            ext.at[fields, both, pl.ds(COLS, HALO), :],
            ext.at[fields, both, pl.ds(0, HALO), :],
            around[0],
        ),
        (
            ext.at[fields, both, pl.ds(HALO, HALO), :],
            ext.at[fields, both, pl.ds(HALO + COLS, HALO), :],
            around[1],
        ),
        (bottom, strips.at[FROM_S], around[2]),
        (top, strips.at[FROM_N], around[3]),
        (own_mask, sides.at[0], around[0]),
        (own_mask, sides.at[1], around[1]),
    ]
    copies = []

    def send(source, target, device):
        number = len(copies)
        copy = pltpu.make_async_remote_copy(
            src_ref=source,
            dst_ref=target,
            send_sem=send_sem.at[number],
            recv_sem=recv_sem.at[number],
            device_id=device,
            device_id_type=MESH,
        )
        copy.start()
        copies.append(copy)

    for source, target, device in sends:
        send(source, target, device)

    size = COLS // 8
    zone = Zone(scratch, [size, size], [1, 0])
    for tile in range(2):
        def load(field, j):
            return ext[field, tile, pl.ds(HALO + j, 8, stride=size), :]

        zone.prepare(tile, load, lambda c: c == COLS - 1, lambda c: own_mask[tile])
        zone.begin(tile, load)
    pairs = [(0, 1)]
    zone.prepare_north((0, 1))
    drives = [DRIVE, jnp.where((zone.lane == LANES - 1) & (lat == n_lat - 1), 0.0, DRIVE)]

    def step(number, carry):
        zone.flows(pairs, drives)
        zone.rivers()
        zone.floods(pairs)
        for k in range(STATE):
            for tile in range(2):
                for j in range(size):
                    inner[number, k, tile, pl.ds(j, 8, stride=size), :] = zone.state[k][
                        zone.base[tile] + j
                    ]
        return carry

    lax.fori_loop(0, STEPS, step, 0)

    for field in range(6):
        values = [
            fold(
                ext[field, 0, HALO + 8 * i : HALO + 8 * i + 8, :],
                ext[field, 1, HALO + 8 * i : HALO + 8 * i + 8, :],
            )
            for i in range(size)
        ]
        for i in range(BAND // 8):
            value = jnp.ones((8, LANES), F32)
            for k in range(4):
                at = 4 * k - 4 + i
                if 0 <= at < size:
                    moved = pltpu.roll(values[at], (32 * k + 8) % LANES, 1)
                    value = jnp.where(zone.lane // 32 == k, moved, value)
            band[field, 8 * i : 8 * i + 8, :] = value

    side_copies = (0, 1, 4, 5)
    for number in side_copies:
        copies[number].wait()
    sixteen = zone.lane // 16
    for side in range(2):
        for i in range(HALO // 8):
            at = 8 * i + (HALO + COLS) * side
            upper = pltpu.roll(sides[side, 0], 96, 1)
            lower = pltpu.roll(sides[side, 1], 112, 1)
            for field in range(6):
                moved = ext[field, 0, at : at + 8, :]
                moved = pltpu.roll(moved, 16 * field, 1) if field else moved
                upper = jnp.where(sixteen == field, moved, upper)
                moved = pltpu.roll(ext[field, 1, at : at + 8, :], 16 * field + 16, 1)
                lower = jnp.where(sixteen == field, moved, lower)
            packed[0, HALO * side + 8 * i : HALO * side + 8 * i + 8, :] = upper
            packed[1, HALO * side + 8 * i : HALO * side + 8 * i + 8, :] = lower
    send(packed.at[1], corners.at[FROM_S], around[2])
    send(packed.at[0], corners.at[FROM_N], around[3])

    zero = jnp.zeros((STRIPS[0], LANES), F32)
    for side in range(2):
        at = pl.ds((WIDE - STRIPS[0]) * side, STRIPS[0])
        for tile in range(2):
            plain[FLOOD, tile, at, :] = ext[DEPTH, tile, at, :]
            plain[LEVEL, tile, at, :] = ext[BED, tile, at, :] + ext[RIVER, tile, at, :]
            for k in (EAST, NORTH, FLUX):
                plain[k, tile, at, :] = zero

    def strip_step(step, shift, strip):
        size = strip // 8
        zone = Zone(scratch, [size] * 4, [1, 0, 3, 2])
        pairs = [(0, 1), (2, 3)]
        starts = (shift, WIDE - strip - shift)
        for side in range(2):
            start = starts[side]
            for tile in range(2):
                t = 2 * side + tile

                def load(field, j):
                    return ext[field, tile, pl.ds(start + j, 8, stride=size), :]

                zone.prepare(
                    t,
                    load,
                    lambda c: (c + start == HALO - 1)
                    | (c + start == HALO + COLS - 1)
                    | (c == strip - 1),
                    lambda c: jnp.where(
                        (c + start < HALO) if side == 0 else (c + start >= HALO + COLS),
                        sides[side, tile],
                        own_mask[tile],
                    ),
                )
                for k in range(STATE):
                    for j in range(size):
                        zone.state[k][zone.base[t] + j] = plain[
                            k, tile, pl.ds(start + j, 8, stride=size), :
                        ]
            zone.prepare_north((2 * side, 2 * side + 1))
        zone.flows(pairs, [drives[0], drives[1], drives[0], drives[1]])
        zone.rivers()
        zone.floods(pairs)
        last = strip != STRIPS[0]
        for side in range(2):
            start = starts[side]
            for tile in range(2):
                t = 2 * side + tile
                for k in range(4 if last else STATE):
                    for j in range(size):
                        plain[k, tile, pl.ds(start + j, 8, stride=size), :] = zone.state[k][
                            zone.base[t] + j
                        ]
                    if last:
                        continue
                    for part in range(2):
                        at = pl.multiple_of(
                            8 * step + 8 * part if side == 0 else 112 - 8 * step + 8 * part, 8
                        )
                        value = inner[step, k, tile, pl.ds(at, 8), :]
                        if part == side and k in (FLOOD, EAST):
                            old = plain[k, tile, pl.ds(HALO + at, 8), :]
                            kept = (zone.sublane == (7 if side else 0)) & (step == 0)
                            value = jnp.where(kept, old, value)
                        plain[k, tile, pl.ds(HALO + at, 8), :] = value

    def early_step(step, carry):
        strip_step(step, 8 * step, STRIPS[0])
        return carry

    lax.fori_loop(0, STEPS - 1, early_step, 0)
    strip_step(STEPS - 1, 16, STRIPS[1])
    for number, copy in enumerate(copies):
        if number not in side_copies:
            copy.wait()


def flow_kernel(
    n_lat,
    ext,
    sides,
    strips,
    corners,
    own_mask,
    inner,
    band,
    plain,
    flood_out,
    river_out,
    east_out,
    north_out,
    rows,
    ends,
    stage,
    sems,
    *scratch,
):
    lat = lax.axis_index("lat")
    wide = BAND // 8
    zone = Zone(scratch, [wide], [0])
    lane, sublane = zone.lane, zone.sublane
    group, place = lane // 32, lane % 32
    halo_lane = (place >= 8) & (place < 24)
    pairs = [(0,)]
    row_closed = ((place == 7) & (lat == n_lat - 1)) | ((place == 23) & (lat == 0))
    drives = [jnp.where(row_closed, 0.0, DRIVE)]
    outs = (flood_out, river_out, east_out, north_out)

    copies = []
    for k in (EAST, NORTH, FLOOD, LEVEL):
        for tile in range(2):
            pieces = []
            for i in range(COLS // 8):
                if 3 <= i < 13:
                    value = inner[STEPS - 1, k, tile, 8 * i : 8 * i + 8, :]
                else:
                    value = plain[k, tile, HALO + 8 * i : HALO + 8 * i + 8, :]
                if k == LEVEL:
                    at = HALO + 8 * i
                    value = jnp.where(
                        own_mask[tile] > 0.0,
                        value - ext[BED, tile, at : at + 8, :],
                        ext[RIVER, tile, at : at + 8, :],
                    )
                pieces.append(value)
            stage[k, tile * LANES : (tile + 1) * LANES, :] = jnp.concatenate(pieces, axis=0).T
        body_rows = pl.ds(8, ROWS - 16)
        copy = pltpu.make_async_copy(stage.at[k, body_rows], outs[k].at[body_rows], sems.at[k])
        copy.start()
        copies.append(copy)

    ones = jnp.ones((8, LANES), F32)
    joined = [
        jnp.where(
            lane % 16 < 8,
            corners[FROM_N, 8 * i : 8 * i + 8, :],
            corners[FROM_S, 8 * i : 8 * i + 8, :],
        )
        for i in range(2 * HALO // 8)
    ]
    for field in range(6):
        pieces = []
        for k in range(4):
            pieces.append(ones)
            for which in (FROM_N, FROM_S):
                value = strips[which, field]
                if k != 1:
                    value = pltpu.roll(value, (160 - 32 * k) % LANES, 1)
                pieces.append(value)
            pieces.append(ones)
        block = jnp.concatenate(pieces, axis=0).T
        for i in range(wide):
            value = band[field, 8 * i : 8 * i + 8, :]
            halo = block[8 * i : 8 * i + 8, :]
            for side, first in ((0, 1), (1, 8)):
                if first <= i < first + 3:
                    ours = group == 3 * side
                    at = 8 * (i - first)
                    moved = pltpu.roll(
                        joined[i - first + 3 * side], (8 + 96 * side - 16 * field) % LANES, 1
                    )
                    halo = jnp.where(ours, moved, halo)
                    at += (HALO + COLS) * side
                    moved = fold(ext[field, 0, at : at + 8, :], ext[field, 1, at : at + 8, :])
                    value = jnp.where(ours, pltpu.roll(moved, 8 + 96 * side, 1), value)
            rows[field, 8 * i : 8 * i + 8, :] = jnp.where(halo_lane, halo, value)

    def row_mask(low, high, halo):
        value = jnp.where(place < 8, pltpu.roll(high, 8, 1), pltpu.roll(low, 24, 1))
        return jnp.where(halo_lane, halo, value)

    middle = row_mask(
        own_mask[0],
        own_mask[1],
        jnp.where(
            place < 16, pltpu.roll(strips[FROM_N, 6], 8, 1), pltpu.roll(strips[FROM_S, 6], 24, 1)
        ),
    )
    west = row_mask(sides[0, 0], sides[0, 1], pltpu.roll(joined[0], 40, 1))
    east = row_mask(sides[1, 0], sides[1, 1], pltpu.roll(joined[3], 40, 1))
    east = pltpu.roll(east, 96, 1)
    spread = middle
    for k in range(1, 4):
        spread = jnp.where(group == k, pltpu.roll(middle, 32 * k, 1), spread)

    def load_row(field, j):
        return rows[field, pl.ds(j, 8, stride=wide), :]

    zone.prepare(
        0,
        load_row,
        lambda c: ((c == 31) & (group == 0)) | ((c == 63) & (group == 3)) | (c == BAND - 1),
        lambda c: jnp.where(
            (c < 32) & (group == 0), west, jnp.where((c >= 64) & (group == 3), east, spread)
        ),
    )
    zone.begin(0, load_row)
    zone.prepare_north((0,))

    def step(_, carry):
        zone.flows(pairs, drives)
        zone.rivers()
        zone.floods(pairs)
        return carry

    lax.fori_loop(0, STEPS, step, 0)

    for k in range(4):
        for j in range(wide):
            ends[k, pl.ds(j, 8, stride=wide), :] = zone.state[k][zone.base[0] + j]
    pieces = []
    for k in range(4):
        for at in range(32, 64, 8):
            value = ends[k, at : at + 8, :]
            if k == LEVEL:
                value = jnp.where(
                    spread > 0.0,
                    value - rows[BED, at : at + 8, :],
                    rows[RIVER, at : at + 8, :],
                )
            pieces.append(value)
    turned = jnp.concatenate(pieces, axis=0).T
    for k in range(4):
        for which in range(2):
            value = None
            for g in range(4):
                at = 32 * g + (24 if which == 0 else 0)
                piece = turned[at : at + 8, :]
                shift = (32 * g - 32 * k) % LANES
                piece = pltpu.roll(piece, shift, 1) if shift else piece
                value = piece if value is None else jnp.where(group == g, piece, value)
            first = 0 if which == 0 else ROWS - 8
            taken = (sublane < 4) if which == 0 else (sublane >= 4)
            end_rows = pl.ds(first, 8)
            stage[k, end_rows, :] = jnp.where(taken, value, stage[k, end_rows, :])
            copy = pltpu.make_async_copy(
                stage.at[k, end_rows], outs[k].at[end_rows], sems.at[4 + 2 * k + which]
            )
            copy.start()
            copies.append(copy)
    for copy in copies:
        copy.wait()


def body(n_lon, n_lat, depth_init, ground, roughness, river_init, reach_mask, width_class, bank_class):
    mask = reach_mask.reshape(2, LANES)
    field = (ROWS, COLS)
    far = pl.BlockSpec(memory_space=pltpu.HBM)
    near = pl.BlockSpec(memory_space=pltpu.VMEM)
    state = [pltpu.VMEM((REGISTERS, 8, LANES), F32)] * SCRATCH
    handed = pl.pallas_call(
        functools.partial(exchange_kernel, n_lon, n_lat),
        out_shape=(
            pltpu.VMEM((6, 2, WIDE, LANES), F32),
            pltpu.VMEM((2, 2, 8, LANES), F32),
            pltpu.VMEM((2, 7, 8, LANES), F32),
            pltpu.VMEM((2, 2 * HALO, LANES), F32),
            pltpu.VMEM((2, 8, LANES), F32),
            pltpu.VMEM((STEPS, STATE, 2, COLS, LANES), F32),
            pltpu.VMEM((6, BAND, LANES), F32),
            pltpu.VMEM((STATE, 2, WIDE, LANES), F32),
        ),
        in_specs=[far] * 7,
        out_specs=(near,) * 8,
        scratch_shapes=[
            pltpu.VMEM((4, ROWS, COLS), F32),
            pltpu.VMEM((2, ROWS, COLS), jnp.int32),
            pltpu.VMEM((2, LANES), jnp.int32),
            pltpu.VMEM((7, 8, LANES), F32),
            pltpu.VMEM((7, 8, LANES), F32),
            pltpu.VMEM((2, 2 * HALO, LANES), F32),
            pltpu.SemaphoreType.DMA((7,)),
            pltpu.SemaphoreType.DMA((8,)),
            pltpu.SemaphoreType.DMA((8,)),
        ]
        + state,
        compiler_params=pltpu.CompilerParams(
            collective_id=0, has_side_effects=True, vmem_limit_bytes=VMEM_LIMIT
        ),
        name="exchange",
    )(*[
        pltpu.with_memory_space_constraint(x, pltpu.HBM)
        for x in (depth_init, ground, roughness, river_init, width_class, bank_class, mask)
    ])
    handed = [pltpu.with_memory_space_constraint(x, pltpu.VMEM) for x in handed]
    return pl.pallas_call(
        functools.partial(flow_kernel, n_lat),
        out_shape=(jax.ShapeDtypeStruct(field, F32),) * 4,
        in_specs=[near] * 8,
        out_specs=(far,) * 4,
        scratch_shapes=[
            pltpu.VMEM((6, BAND, LANES), F32),
            pltpu.VMEM((4, BAND, LANES), F32),
            pltpu.VMEM((4, ROWS, COLS), F32),
            pltpu.SemaphoreType.DMA((12,)),
        ]
        + state,
        compiler_params=pltpu.CompilerParams(vmem_limit_bytes=VMEM_LIMIT),
        name="flow",
    )(*handed)


def solution(mesh):
    placed = P("lat", "lon")
    return jax.shard_map(
        functools.partial(body, mesh.shape["lon"], mesh.shape["lat"]),
        mesh=mesh,
        in_specs=(placed,) * 7,
        out_specs=(placed,) * 4,
        check_vma=False,
    )
```

```python
import functools
import math

import jax
import jax.numpy as jnp
from jax import lax
from jax.experimental import pallas as pl
from jax.experimental.pallas import tpu as pltpu
from jax.sharding import PartitionSpec as P

MESH = pl.DeviceIdType.MESH
F32 = jnp.float32
SUB = 8
STEPS = 4
ROWS = 256
COLS = 128
HALO = 24
WIDE = COLS + 2 * HALO
LANES = 128
STRIPS = (32, 40)
BAND = 96
DEPTH, GROUND, ROUGH, RIVER, WIDTH, BED = range(6)
FROM_S, FROM_N = range(2)
FLOOD, LEVEL, EAST, NORTH, FLUX = range(5)

GRAVITY = 9.81
CELL_SIZE = 90.0
TIME_STEP = 10.0
SHALLOW = 0.1
EXCHANGE = 0.01
CHANNEL_MANNING = 0.035
SHORT_STEP = TIME_STEP / SUB
POWER = -7.0 / 6.0 / math.log(2.0)
DRIVE = GRAVITY * TIME_STEP / CELL_SIZE

STATE = 5
SCRATCH = 17
REGISTERS = 32
UNROLL = 8
VMEM_LIMIT = 24 << 20


def quotient(current, height, drop, friction, drive):
    power = jnp.exp2(POWER * jnp.log(height * height + SHALLOW * SHALLOW))
    resisted = 1.0 + friction * jnp.abs(current) * power
    return (current - drive * (height * drop)) / resisted


class Zone:
    def __init__(self, refs, sizes, partners):
        self.sizes = sizes
        self.partners = partners
        self.base = [sum(sizes[:t]) for t in range(len(sizes))]
        self.state = refs[:STATE]
        (
            self.g,
            self.sur,
            self.e_base,
            self.e_fric,
            self.n_base,
            self.n_fric,
            self.r_base,
            self.r_drive,
            self.r_fric,
            self.r_inv,
            self.give,
            self.total,
        ) = refs[STATE:]
        self.lane = lax.broadcasted_iota(jnp.int32, (8, LANES), 1)
        self.sublane = lax.broadcasted_iota(jnp.int32, (8, LANES), 0)

    def column(self, tile, j):
        return self.sublane * self.sizes[tile] + j

    def northward(self, read, tile):
        here = pltpu.roll(read(tile), LANES - 1, 1)
        if self.partners[tile] == tile:
            return here
        there = pltpu.roll(read(self.partners[tile]), LANES - 1, 1)
        return jnp.where(self.lane == LANES - 1, there, here)

    def southward(self, read, tile):
        here = pltpu.roll(read(tile), 1, 1)
        if self.partners[tile] == tile:
            return here
        there = pltpu.roll(read(self.partners[tile]), 1, 1)
        return jnp.where(self.lane == 0, there, here)

    def prepare(self, tile, load, closed, mask):
        size, base = self.sizes[tile], self.base[tile]

        def after(values, j):
            return values[j + 1] if j + 1 < size else pltpu.roll(values[0], 7, 0)

        grounds = [load(GROUND, j) for j in range(size)]
        roughs = [load(ROUGH, j) for j in range(size)]
        beds = [load(BED, j) for j in range(size)]
        widths = [load(WIDTH, j) for j in range(size)]
        for j in range(size):
            at = base + j
            column = self.column(tile, j)
            self.g[at] = grounds[j]
            self.e_base[at] = jnp.maximum(grounds[j], after(grounds, j))
            self.e_fric[at] = (GRAVITY * TIME_STEP) * (roughs[j] * after(roughs, j))
            self.n_fric[at] = roughs[j]
            breadth = 0.5 * (widths[j] + after(widths, j))
            self.r_base[at] = jnp.maximum(beds[j], after(beds, j))
            self.r_drive[at] = jnp.where(
                closed(column), 0.0, (GRAVITY * SHORT_STEP / CELL_SIZE) * breadth
            )
            self.r_fric[at] = (
                GRAVITY * SHORT_STEP * CHANNEL_MANNING * CHANNEL_MANNING
            ) / breadth
            self.r_inv[at] = SHORT_STEP / (CELL_SIZE * widths[j])
            self.give[at] = mask(column) * widths[j] * (SHORT_STEP * EXCHANGE / CELL_SIZE)

    def prepare_north(self, tiles):
        for j in range(self.sizes[tiles[0]]):
            grounds = {t: self.g[self.base[t] + j] for t in tiles}
            roughs = {t: self.n_fric[self.base[t] + j] for t in tiles}
            for t in tiles:
                at = self.base[t] + j
                self.n_base[at] = jnp.maximum(grounds[t], self.northward(grounds.get, t))
                self.n_fric[at] = (GRAVITY * TIME_STEP) * (
                    roughs[t] * self.northward(roughs.get, t)
                )

    def begin(self, tile, load):
        for j in range(self.sizes[tile]):
            at = self.base[tile] + j
            self.state[FLOOD][at] = load(DEPTH, j)
            self.state[LEVEL][at] = load(BED, j) + load(RIVER, j)
            for k in (EAST, NORTH, FLUX):
                self.state[k][at] = jnp.zeros((8, LANES), F32)

    def flows(self, pairs, drives):
        flood, _, q_east, q_north, _ = self.state
        for tiles in pairs:
            for t in tiles:
                for j in range(self.sizes[t]):
                    at = self.base[t] + j
                    self.sur[at] = self.g[at] + flood[at]
                    self.total[at] = jnp.zeros((8, LANES), F32)
        for tiles in pairs:
            for t in tiles:
                base, size = self.base[t], self.sizes[t]
                for j in range(size):
                    here = self.sur[base + j]
                    there = (
                        self.sur[base + j + 1] if j + 1 < size else pltpu.roll(self.sur[base], 7, 0)
                    )
                    q_east[base + j] = quotient(
                        q_east[base + j],
                        jnp.maximum(here, there) - self.e_base[base + j],
                        there - here,
                        self.e_fric[base + j],
                        DRIVE,
                    )
        for tiles in pairs:
            for j in range(self.sizes[tiles[0]]):
                surfaces = {t: self.sur[self.base[t] + j] for t in tiles}
                for t in tiles:
                    at = self.base[t] + j
                    there = self.northward(surfaces.get, t)
                    q_north[at] = quotient(
                        q_north[at],
                        jnp.maximum(surfaces[t], there) - self.n_base[at],
                        there - surfaces[t],
                        self.n_fric[at],
                        drives[t],
                    )

    def rivers(self):
        level, flux = self.state[LEVEL], self.state[FLUX]
        rate = SHORT_STEP * EXCHANGE

        if sum(self.sizes) > 20:
            return self.rivers_in_memory()
        count = sum(self.sizes)

        def substep(_, carry):
            levels, fluxes = list(carry[:count]), list(carry[count:])
            outs = [None] * count
            for t, size in enumerate(self.sizes):
                base = self.base[t]
                for j in range(size):
                    at = base + j
                    here = levels[at]
                    there = levels[at + 1] if j + 1 < size else pltpu.roll(levels[base], 7, 0)
                    outs[at] = quotient(
                        fluxes[at],
                        jnp.maximum(here, there) - self.r_base[at],
                        there - here,
                        self.r_fric[at],
                        self.r_drive[at],
                    )
                    self.total[at] += here
            fresh = []
            for t, size in enumerate(self.sizes):
                base = self.base[t]
                for j in range(size):
                    at = base + j
                    west = outs[at - 1] if j else pltpu.roll(outs[base + size - 1], 1, 0)
                    fresh.append(
                        (1.0 - rate) * levels[at]
                        + (rate * self.sur[at] + (west - outs[at]) * self.r_inv[at])
                    )
            return tuple(fresh) + tuple(outs)

        start = [level[at] for at in range(count)] + [flux[at] for at in range(count)]
        final = lax.fori_loop(0, SUB, substep, tuple(start), unroll=UNROLL)
        for at in range(count):
            level[at] = final[at]
            flux[at] = final[count + at]

    def rivers_in_memory(self):
        level, flux = self.state[LEVEL], self.state[FLUX]
        rate = SHORT_STEP * EXCHANGE

        def substep(_, carry):
            for t, size in enumerate(self.sizes):
                base = self.base[t]
                first = level[base]
                here = first
                first_flux = None
                last_flux = None
                for j in range(size):
                    at = base + j
                    there = level[at + 1] if j + 1 < size else pltpu.roll(first, 7, 0)
                    out = quotient(
                        flux[at],
                        jnp.maximum(here, there) - self.r_base[at],
                        there - here,
                        self.r_fric[at],
                        self.r_drive[at],
                    )
                    flux[at] = out
                    self.total[at] += here
                    if j:
                        level[at] = (
                            here
                            - rate * (here - self.sur[at])
                            + (last_flux - out) * self.r_inv[at]
                        )
                    else:
                        first_flux = out
                    last_flux = out
                    here = there
                level[base] = (
                    first
                    - rate * (first - self.sur[base])
                    + (pltpu.roll(last_flux, 1, 0) - first_flux) * self.r_inv[base]
                )
            return carry

        lax.fori_loop(0, SUB, substep, 0)

    def floods(self, pairs):
        flood, _, q_east, q_north, _ = self.state
        for tiles in pairs:
            for j in range(self.sizes[tiles[0]]):
                norths = {t: q_north[self.base[t] + j] for t in tiles}
                for t in tiles:
                    base, size = self.base[t], self.sizes[t]
                    at = base + j
                    west = q_east[at - 1] if j else pltpu.roll(q_east[base + size - 1], 1, 0)
                    flooded = flood[at] + (TIME_STEP / CELL_SIZE) * (
                        west - q_east[at] + self.southward(norths.get, t) - norths[t]
                    )
                    flood[at] = flooded + self.give[at] * (self.total[at] - SUB * self.sur[at])


def fold(low, high):
    lane = lax.broadcasted_iota(jnp.int32, (8, LANES), 1)
    return jnp.where(lane < 64, pltpu.roll(low, 16, 1), high)


def exchange_kernel(
    n_lon,
    n_lat,
    depth_hbm,
    ground_hbm,
    rough_hbm,
    river_hbm,
    width_hbm,
    bank_hbm,
    mask_hbm,
    ext,
    sides,
    strips,
    corners,
    own_mask,
    inner,
    band,
    plain,
    floats,
    ints,
    mask_in,
    top,
    bottom,
    packed,
    load_sem,
    send_sem,
    recv_sem,
    *scratch,
):
    lon = lax.axis_index("lon")
    lat = lax.axis_index("lat")
    east = lax.rem(lon + 1, n_lon)
    west = lax.rem(lon + n_lon - 1, n_lon)
    north = lax.rem(lat + 1, n_lat)
    south = lax.rem(lat + n_lat - 1, n_lat)
    around = [
        (east, lat),
        (west, lat),
        (lon, north),
        (lon, south),
    ]
    around = [{"lon": a, "lat": b} for a, b in around]
    barrier = pltpu.get_barrier_semaphore()
    for device in around:
        pl.semaphore_signal(barrier, inc=1, device_id=device, device_id_type=MESH)

    loads = []
    for number, (source, target) in enumerate(
        [
            (ground_hbm, floats.at[GROUND]),
            (bank_hbm, ints.at[0]),
            (width_hbm, ints.at[1]),
            (river_hbm, floats.at[RIVER]),
            (depth_hbm, floats.at[DEPTH]),
            (rough_hbm, floats.at[ROUGH]),
            (mask_hbm, mask_in),
        ]
    ):
        copy = pltpu.make_async_copy(source, target, load_sem.at[number])
        copy.start()
        loads.append(copy)

    def place(field, values):
        for tile in range(2):
            ext[field, tile, HALO : HALO + COLS, :] = values[tile * LANES : (tile + 1) * LANES, :].T
        top[field] = values[0:8, :]
        bottom[field] = values[ROWS - 8 : ROWS, :]

    loads[0].wait()
    ground = floats[GROUND]
    place(GROUND, ground)
    loads[1].wait()
    place(BED, ground - (1.0 + 0.5 * ints[0].astype(F32)))
    loads[2].wait()
    place(WIDTH, 8.0 + 9.0 * ints[1].astype(F32))
    loads[3].wait()
    place(RIVER, floats[RIVER])
    loads[4].wait()
    place(DEPTH, floats[DEPTH])
    loads[5].wait()
    place(ROUGH, floats[ROUGH])
    loads[6].wait()
    for tile in range(2):
        own_mask[tile] = jnp.broadcast_to(mask_in[tile : tile + 1, :].astype(F32), (8, LANES))
    top[6] = own_mask[0]
    bottom[6] = own_mask[1]

    pl.semaphore_wait(barrier, len(around))
    fields = pl.ds(0, 6)
    both = pl.ds(0, 2)
    sends = [
        (
            ext.at[fields, both, pl.ds(COLS, HALO), :],
            ext.at[fields, both, pl.ds(0, HALO), :],
            around[0],
        ),
        (
            ext.at[fields, both, pl.ds(HALO, HALO), :],
            ext.at[fields, both, pl.ds(HALO + COLS, HALO), :],
            around[1],
        ),
        (bottom, strips.at[FROM_S], around[2]),
        (top, strips.at[FROM_N], around[3]),
        (own_mask, sides.at[0], around[0]),
        (own_mask, sides.at[1], around[1]),
    ]
    copies = []

    def send(source, target, device):
        number = len(copies)
        copy = pltpu.make_async_remote_copy(
            src_ref=source,
            dst_ref=target,
            send_sem=send_sem.at[number],
            recv_sem=recv_sem.at[number],
            device_id=device,
            device_id_type=MESH,
        )
        copy.start()
        copies.append(copy)

    for source, target, device in sends:
        send(source, target, device)

    size = COLS // 8
    zone = Zone(scratch, [size, size], [1, 0])
    for tile in range(2):
        def load(field, j):
            return ext[field, tile, pl.ds(HALO + j, 8, stride=size), :]

        zone.prepare(tile, load, lambda c: c == COLS - 1, lambda c: own_mask[tile])
        zone.begin(tile, load)
    pairs = [(0, 1)]
    zone.prepare_north((0, 1))
    drives = [DRIVE, jnp.where((zone.lane == LANES - 1) & (lat == n_lat - 1), 0.0, DRIVE)]

    def step(number, carry):
        zone.flows(pairs, drives)
        zone.rivers()
        zone.floods(pairs)
        for k in range(STATE):
            for tile in range(2):
                for j in range(size):
                    inner[number, k, tile, pl.ds(j, 8, stride=size), :] = zone.state[k][
                        zone.base[tile] + j
                    ]
        return carry

    lax.fori_loop(0, STEPS, step, 0)

    for field in range(6):
        values = [
            fold(
                ext[field, 0, HALO + 8 * i : HALO + 8 * i + 8, :],
                ext[field, 1, HALO + 8 * i : HALO + 8 * i + 8, :],
            )
            for i in range(size)
        ]
        for i in range(BAND // 8):
            value = jnp.ones((8, LANES), F32)
            for k in range(4):
                at = 4 * k - 4 + i
                if 0 <= at < size:
                    moved = pltpu.roll(values[at], (32 * k + 8) % LANES, 1)
                    value = jnp.where(zone.lane // 32 == k, moved, value)
            band[field, 8 * i : 8 * i + 8, :] = value

    side_copies = (0, 1, 4, 5)
    for number in side_copies:
        copies[number].wait()
    sixteen = zone.lane // 16
    for side in range(2):
        for i in range(HALO // 8):
            at = 8 * i + (HALO + COLS) * side
            upper = pltpu.roll(sides[side, 0], 96, 1)
            lower = pltpu.roll(sides[side, 1], 112, 1)
            for field in range(6):
                moved = ext[field, 0, at : at + 8, :]
                moved = pltpu.roll(moved, 16 * field, 1) if field else moved
                upper = jnp.where(sixteen == field, moved, upper)
                moved = pltpu.roll(ext[field, 1, at : at + 8, :], 16 * field + 16, 1)
                lower = jnp.where(sixteen == field, moved, lower)
            packed[0, HALO * side + 8 * i : HALO * side + 8 * i + 8, :] = upper
            packed[1, HALO * side + 8 * i : HALO * side + 8 * i + 8, :] = lower
    send(packed.at[1], corners.at[FROM_S], around[2])
    send(packed.at[0], corners.at[FROM_N], around[3])

    zero = jnp.zeros((STRIPS[0], LANES), F32)
    for side in range(2):
        at = pl.ds((WIDE - STRIPS[0]) * side, STRIPS[0])
        for tile in range(2):
            plain[FLOOD, tile, at, :] = ext[DEPTH, tile, at, :]
            plain[LEVEL, tile, at, :] = ext[BED, tile, at, :] + ext[RIVER, tile, at, :]
            for k in (EAST, NORTH, FLUX):
                plain[k, tile, at, :] = zero

    def strip_step(step, shift, strip):
        size = strip // 8
        zone = Zone(scratch, [size] * 4, [1, 0, 3, 2])
        pairs = [(0, 1), (2, 3)]
        starts = (shift, WIDE - strip - shift)
        for side in range(2):
            start = starts[side]
            for tile in range(2):
                t = 2 * side + tile

                def load(field, j):
                    return ext[field, tile, pl.ds(start + j, 8, stride=size), :]

                zone.prepare(
                    t,
                    load,
                    lambda c: (c + start == HALO - 1)
                    | (c + start == HALO + COLS - 1)
                    | (c == strip - 1),
                    lambda c: jnp.where(
                        (c + start < HALO) if side == 0 else (c + start >= HALO + COLS),
                        sides[side, tile],
                        own_mask[tile],
                    ),
                )
                for k in range(STATE):
                    for j in range(size):
                        zone.state[k][zone.base[t] + j] = plain[
                            k, tile, pl.ds(start + j, 8, stride=size), :
                        ]
            zone.prepare_north((2 * side, 2 * side + 1))
        zone.flows(pairs, [drives[0], drives[1], drives[0], drives[1]])
        zone.rivers()
        zone.floods(pairs)
        last = strip != STRIPS[0]
        for side in range(2):
            start = starts[side]
            for tile in range(2):
                t = 2 * side + tile
                for k in range(4 if last else STATE):
                    for j in range(size):
                        plain[k, tile, pl.ds(start + j, 8, stride=size), :] = zone.state[k][
                            zone.base[t] + j
                        ]
                    if last:
                        continue
                    for part in range(2):
                        at = pl.multiple_of(
                            8 * step + 8 * part if side == 0 else 112 - 8 * step + 8 * part, 8
                        )
                        value = inner[step, k, tile, pl.ds(at, 8), :]
                        if part == side and k in (FLOOD, EAST):
                            old = plain[k, tile, pl.ds(HALO + at, 8), :]
                            kept = (zone.sublane == (7 if side else 0)) & (step == 0)
                            value = jnp.where(kept, old, value)
                        plain[k, tile, pl.ds(HALO + at, 8), :] = value

    for step in range(STEPS - 1):
        strip_step(step, 8 * step, STRIPS[0])
    strip_step(STEPS - 1, 16, STRIPS[1])
    for number, copy in enumerate(copies):
        if number not in side_copies:
            copy.wait()


def flow_kernel(
    n_lat,
    ext,
    sides,
    strips,
    corners,
    own_mask,
    inner,
    band,
    plain,
    flood_out,
    river_out,
    east_out,
    north_out,
    rows,
    ends,
    stage,
    sems,
    *scratch,
):
    lat = lax.axis_index("lat")
    wide = BAND // 8
    zone = Zone(scratch, [wide], [0])
    lane, sublane = zone.lane, zone.sublane
    group, place = lane // 32, lane % 32
    halo_lane = (place >= 8) & (place < 24)
    pairs = [(0,)]
    row_closed = ((place == 7) & (lat == n_lat - 1)) | ((place == 23) & (lat == 0))
    drives = [jnp.where(row_closed, 0.0, DRIVE)]
    outs = (flood_out, river_out, east_out, north_out)

    copies = []
    for k in (EAST, NORTH, FLOOD, LEVEL):
        for tile in range(2):
            pieces = []
            for i in range(COLS // 8):
                if 3 <= i < 13:
                    value = inner[STEPS - 1, k, tile, 8 * i : 8 * i + 8, :]
                else:
                    value = plain[k, tile, HALO + 8 * i : HALO + 8 * i + 8, :]
                if k == LEVEL:
                    at = HALO + 8 * i
                    value = jnp.where(
                        own_mask[tile] > 0.0,
                        value - ext[BED, tile, at : at + 8, :],
                        ext[RIVER, tile, at : at + 8, :],
                    )
                pieces.append(value)
            stage[k, tile * LANES : (tile + 1) * LANES, :] = jnp.concatenate(pieces, axis=0).T
        body_rows = pl.ds(8, ROWS - 16)
        copy = pltpu.make_async_copy(stage.at[k, body_rows], outs[k].at[body_rows], sems.at[k])
        copy.start()
        copies.append(copy)

    ones = jnp.ones((8, LANES), F32)
    joined = [
        jnp.where(
            lane % 16 < 8,
            corners[FROM_N, 8 * i : 8 * i + 8, :],
            corners[FROM_S, 8 * i : 8 * i + 8, :],
        )
        for i in range(2 * HALO // 8)
    ]
    for field in range(6):
        pieces = []
        for k in range(4):
            pieces.append(ones)
            for which in (FROM_N, FROM_S):
                value = strips[which, field]
                if k != 1:
                    value = pltpu.roll(value, (160 - 32 * k) % LANES, 1)
                pieces.append(value)
            pieces.append(ones)
        block = jnp.concatenate(pieces, axis=0).T
        for i in range(wide):
            value = band[field, 8 * i : 8 * i + 8, :]
            halo = block[8 * i : 8 * i + 8, :]
            for side, first in ((0, 1), (1, 8)):
                if first <= i < first + 3:
                    ours = group == 3 * side
                    at = 8 * (i - first)
                    moved = pltpu.roll(
                        joined[i - first + 3 * side], (8 + 96 * side - 16 * field) % LANES, 1
                    )
                    halo = jnp.where(ours, moved, halo)
                    at += (HALO + COLS) * side
                    moved = fold(ext[field, 0, at : at + 8, :], ext[field, 1, at : at + 8, :])
                    value = jnp.where(ours, pltpu.roll(moved, 8 + 96 * side, 1), value)
            rows[field, 8 * i : 8 * i + 8, :] = jnp.where(halo_lane, halo, value)

    def row_mask(low, high, halo):
        value = jnp.where(place < 8, pltpu.roll(high, 8, 1), pltpu.roll(low, 24, 1))
        return jnp.where(halo_lane, halo, value)

    middle = row_mask(
        own_mask[0],
        own_mask[1],
        jnp.where(
            place < 16, pltpu.roll(strips[FROM_N, 6], 8, 1), pltpu.roll(strips[FROM_S, 6], 24, 1)
        ),
    )
    west = row_mask(sides[0, 0], sides[0, 1], pltpu.roll(joined[0], 40, 1))
    east = row_mask(sides[1, 0], sides[1, 1], pltpu.roll(joined[3], 40, 1))
    east = pltpu.roll(east, 96, 1)
    spread = middle
    for k in range(1, 4):
        spread = jnp.where(group == k, pltpu.roll(middle, 32 * k, 1), spread)

    def load_row(field, j):
        return rows[field, pl.ds(j, 8, stride=wide), :]

    zone.prepare(
        0,
        load_row,
        lambda c: ((c == 31) & (group == 0)) | ((c == 63) & (group == 3)) | (c == BAND - 1),
        lambda c: jnp.where(
            (c < 32) & (group == 0), west, jnp.where((c >= 64) & (group == 3), east, spread)
        ),
    )
    zone.begin(0, load_row)
    zone.prepare_north((0,))

    def step(_, carry):
        zone.flows(pairs, drives)
        zone.rivers()
        zone.floods(pairs)
        return carry

    for _ in range(STEPS):
        step(_, 0)

    for k in range(4):
        for j in range(wide):
            ends[k, pl.ds(j, 8, stride=wide), :] = zone.state[k][zone.base[0] + j]
    pieces = []
    for k in range(4):
        for at in range(32, 64, 8):
            value = ends[k, at : at + 8, :]
            if k == LEVEL:
                value = jnp.where(
                    spread > 0.0,
                    value - rows[BED, at : at + 8, :],
                    rows[RIVER, at : at + 8, :],
                )
            pieces.append(value)
    turned = jnp.concatenate(pieces, axis=0).T
    for k in range(4):
        for which in range(2):
            value = None
            for g in range(4):
                at = 32 * g + (24 if which == 0 else 0)
                piece = turned[at : at + 8, :]
                shift = (32 * g - 32 * k) % LANES
                piece = pltpu.roll(piece, shift, 1) if shift else piece
                value = piece if value is None else jnp.where(group == g, piece, value)
            first = 0 if which == 0 else ROWS - 8
            taken = (sublane < 4) if which == 0 else (sublane >= 4)
            end_rows = pl.ds(first, 8)
            stage[k, end_rows, :] = jnp.where(taken, value, stage[k, end_rows, :])
            copy = pltpu.make_async_copy(
                stage.at[k, end_rows], outs[k].at[end_rows], sems.at[4 + 2 * k + which]
            )
            copy.start()
            copies.append(copy)
    for copy in copies:
        copy.wait()


def body(n_lon, n_lat, depth_init, ground, roughness, river_init, reach_mask, width_class, bank_class):
    mask = reach_mask.reshape(2, LANES)
    field = (ROWS, COLS)
    far = pl.BlockSpec(memory_space=pltpu.HBM)
    near = pl.BlockSpec(memory_space=pltpu.VMEM)
    state = [pltpu.VMEM((REGISTERS, 8, LANES), F32)] * SCRATCH
    handed = pl.pallas_call(
        functools.partial(exchange_kernel, n_lon, n_lat),
        out_shape=(
            pltpu.VMEM((6, 2, WIDE, LANES), F32),
            pltpu.VMEM((2, 2, 8, LANES), F32),
            pltpu.VMEM((2, 7, 8, LANES), F32),
            pltpu.VMEM((2, 2 * HALO, LANES), F32),
            pltpu.VMEM((2, 8, LANES), F32),
            pltpu.VMEM((STEPS, STATE, 2, COLS, LANES), F32),
            pltpu.VMEM((6, BAND, LANES), F32),
            pltpu.VMEM((STATE, 2, WIDE, LANES), F32),
        ),
        in_specs=[far] * 7,
        out_specs=(near,) * 8,
        scratch_shapes=[
            pltpu.VMEM((4, ROWS, COLS), F32),
            pltpu.VMEM((2, ROWS, COLS), jnp.int32),
            pltpu.VMEM((2, LANES), jnp.int32),
            pltpu.VMEM((7, 8, LANES), F32),
            pltpu.VMEM((7, 8, LANES), F32),
            pltpu.VMEM((2, 2 * HALO, LANES), F32),
            pltpu.SemaphoreType.DMA((7,)),
            pltpu.SemaphoreType.DMA((8,)),
            pltpu.SemaphoreType.DMA((8,)),
        ]
        + state,
        compiler_params=pltpu.CompilerParams(
            collective_id=0, has_side_effects=True, vmem_limit_bytes=VMEM_LIMIT
        ),
        name="exchange",
    )(*[
        pltpu.with_memory_space_constraint(x, pltpu.HBM)
        for x in (depth_init, ground, roughness, river_init, width_class, bank_class, mask)
    ])
    handed = [pltpu.with_memory_space_constraint(x, pltpu.VMEM) for x in handed]
    return pl.pallas_call(
        functools.partial(flow_kernel, n_lat),
        out_shape=(jax.ShapeDtypeStruct(field, F32),) * 4,
        in_specs=[near] * 8,
        out_specs=(far,) * 4,
        scratch_shapes=[
            pltpu.VMEM((6, BAND, LANES), F32),
            pltpu.VMEM((4, BAND, LANES), F32),
            pltpu.VMEM((4, ROWS, COLS), F32),
            pltpu.SemaphoreType.DMA((12,)),
        ]
        + state,
        compiler_params=pltpu.CompilerParams(vmem_limit_bytes=VMEM_LIMIT),
        name="flow",
    )(*handed)


def solution(mesh):
    placed = P("lat", "lon")
    return jax.shard_map(
        functools.partial(body, mesh.shape["lon"], mesh.shape["lat"]),
        mesh=mesh,
        in_specs=(placed,) * 7,
        out_specs=(placed,) * 4,
        check_vma=False,
    )
```

```python
import functools
import math

import jax
import jax.numpy as jnp
from jax import lax
from jax.experimental import pallas as pl
from jax.experimental.pallas import tpu as pltpu
from jax.sharding import PartitionSpec as P

MESH = pl.DeviceIdType.MESH
F32 = jnp.float32
SUB = 8
STEPS = 4
ROWS = 256
COLS = 128
HALO = 24
WIDE = COLS + 2 * HALO
LANES = 128
STRIPS = (32, 40)
BAND = 96
DEPTH, GROUND, ROUGH, RIVER, WIDTH, BED = range(6)
FROM_S, FROM_N = range(2)
FLOOD, LEVEL, EAST, NORTH, FLUX = range(5)

GRAVITY = 9.81
CELL_SIZE = 90.0
TIME_STEP = 10.0
SHALLOW = 0.1
EXCHANGE = 0.01
CHANNEL_MANNING = 0.035
SHORT_STEP = TIME_STEP / SUB
POWER = -7.0 / 6.0 / math.log(2.0)
DRIVE = GRAVITY * TIME_STEP / CELL_SIZE

STATE = 5
SCRATCH = 17
REGISTERS = 32
UNROLL = 8
VMEM_LIMIT = 24 << 20


def quotient(current, height, drop, friction, drive):
    power = jnp.exp2(POWER * jnp.log(height * height + SHALLOW * SHALLOW))
    resisted = 1.0 + friction * jnp.abs(current) * power
    return (current - drive * (height * drop)) / resisted


class Zone:
    def __init__(self, refs, sizes, partners):
        self.sizes = sizes
        self.partners = partners
        self.base = [sum(sizes[:t]) for t in range(len(sizes))]
        self.state = refs[:STATE]
        (
            self.g,
            self.sur,
            self.e_base,
            self.e_fric,
            self.n_base,
            self.n_fric,
            self.r_base,
            self.r_drive,
            self.r_fric,
            self.r_inv,
            self.give,
            self.total,
        ) = refs[STATE:]
        self.lane = lax.broadcasted_iota(jnp.int32, (8, LANES), 1)
        self.sublane = lax.broadcasted_iota(jnp.int32, (8, LANES), 0)

    def column(self, tile, j):
        return self.sublane * self.sizes[tile] + j

    def northward(self, read, tile):
        here = pltpu.roll(read(tile), LANES - 1, 1)
        if self.partners[tile] == tile:
            return here
        there = pltpu.roll(read(self.partners[tile]), LANES - 1, 1)
        return jnp.where(self.lane == LANES - 1, there, here)

    def southward(self, read, tile):
        here = pltpu.roll(read(tile), 1, 1)
        if self.partners[tile] == tile:
            return here
        there = pltpu.roll(read(self.partners[tile]), 1, 1)
        return jnp.where(self.lane == 0, there, here)

    def prepare(self, tile, load, closed, mask):
        size, base = self.sizes[tile], self.base[tile]

        def after(values, j):
            return values[j + 1] if j + 1 < size else pltpu.roll(values[0], 7, 0)

        grounds = [load(GROUND, j) for j in range(size)]
        roughs = [load(ROUGH, j) for j in range(size)]
        beds = [load(BED, j) for j in range(size)]
        widths = [load(WIDTH, j) for j in range(size)]
        for j in range(size):
            at = base + j
            column = self.column(tile, j)
            self.g[at] = grounds[j]
            self.e_base[at] = jnp.maximum(grounds[j], after(grounds, j))
            self.e_fric[at] = (GRAVITY * TIME_STEP) * (roughs[j] * after(roughs, j))
            self.n_fric[at] = roughs[j]
            breadth = 0.5 * (widths[j] + after(widths, j))
            self.r_base[at] = jnp.maximum(beds[j], after(beds, j))
            self.r_drive[at] = jnp.where(
                closed(column), 0.0, (GRAVITY * SHORT_STEP / CELL_SIZE) * breadth
            )
            self.r_fric[at] = (
                GRAVITY * SHORT_STEP * CHANNEL_MANNING * CHANNEL_MANNING
            ) / breadth
            self.r_inv[at] = SHORT_STEP / (CELL_SIZE * widths[j])
            self.give[at] = mask(column) * widths[j] * (SHORT_STEP * EXCHANGE / CELL_SIZE)

    def prepare_north(self, tiles):
        for j in range(self.sizes[tiles[0]]):
            grounds = {t: self.g[self.base[t] + j] for t in tiles}
            roughs = {t: self.n_fric[self.base[t] + j] for t in tiles}
            for t in tiles:
                at = self.base[t] + j
                self.n_base[at] = jnp.maximum(grounds[t], self.northward(grounds.get, t))
                self.n_fric[at] = (GRAVITY * TIME_STEP) * (
                    roughs[t] * self.northward(roughs.get, t)
                )

    def begin(self, tile, load):
        for j in range(self.sizes[tile]):
            at = self.base[tile] + j
            self.state[FLOOD][at] = load(DEPTH, j)
            self.state[LEVEL][at] = load(BED, j) + load(RIVER, j)
            for k in (EAST, NORTH, FLUX):
                self.state[k][at] = jnp.zeros((8, LANES), F32)

    def flows(self, pairs, drives):
        flood, _, q_east, q_north, _ = self.state
        for tiles in pairs:
            for t in tiles:
                for j in range(self.sizes[t]):
                    at = self.base[t] + j
                    self.sur[at] = self.g[at] + flood[at]
                    self.total[at] = jnp.zeros((8, LANES), F32)
        for tiles in pairs:
            for t in tiles:
                base, size = self.base[t], self.sizes[t]
                for j in range(size):
                    here = self.sur[base + j]
                    there = (
                        self.sur[base + j + 1] if j + 1 < size else pltpu.roll(self.sur[base], 7, 0)
                    )
                    q_east[base + j] = quotient(
                        q_east[base + j],
                        jnp.maximum(here, there) - self.e_base[base + j],
                        there - here,
                        self.e_fric[base + j],
                        DRIVE,
                    )
        for tiles in pairs:
            for j in range(self.sizes[tiles[0]]):
                surfaces = {t: self.sur[self.base[t] + j] for t in tiles}
                for t in tiles:
                    at = self.base[t] + j
                    there = self.northward(surfaces.get, t)
                    q_north[at] = quotient(
                        q_north[at],
                        jnp.maximum(surfaces[t], there) - self.n_base[at],
                        there - surfaces[t],
                        self.n_fric[at],
                        drives[t],
                    )

    def rivers(self):
        level, flux = self.state[LEVEL], self.state[FLUX]
        rate = SHORT_STEP * EXCHANGE

        if sum(self.sizes) > 20:
            return self.rivers_in_memory()
        count = sum(self.sizes)

        def substep(_, carry):
            levels, fluxes = list(carry[:count]), list(carry[count:])
            outs = [None] * count
            for t, size in enumerate(self.sizes):
                base = self.base[t]
                for j in range(size):
                    at = base + j
                    here = levels[at]
                    there = levels[at + 1] if j + 1 < size else pltpu.roll(levels[base], 7, 0)
                    outs[at] = quotient(
                        fluxes[at],
                        jnp.maximum(here, there) - self.r_base[at],
                        there - here,
                        self.r_fric[at],
                        self.r_drive[at],
                    )
                    self.total[at] += here
            fresh = []
            for t, size in enumerate(self.sizes):
                base = self.base[t]
                for j in range(size):
                    at = base + j
                    west = outs[at - 1] if j else pltpu.roll(outs[base + size - 1], 1, 0)
                    fresh.append(
                        (1.0 - rate) * levels[at]
                        + (rate * self.sur[at] + (west - outs[at]) * self.r_inv[at])
                    )
            return tuple(fresh) + tuple(outs)

        start = [level[at] for at in range(count)] + [flux[at] for at in range(count)]
        final = lax.fori_loop(0, SUB, substep, tuple(start), unroll=UNROLL)
        for at in range(count):
            level[at] = final[at]
            flux[at] = final[count + at]

    def rivers_in_memory(self):
        level, flux = self.state[LEVEL], self.state[FLUX]
        rate = SHORT_STEP * EXCHANGE

        def substep(_, carry):
            for t, size in enumerate(self.sizes):
                base = self.base[t]
                first = level[base]
                here = first
                first_flux = None
                last_flux = None
                for j in range(size):
                    at = base + j
                    there = level[at + 1] if j + 1 < size else pltpu.roll(first, 7, 0)
                    out = quotient(
                        flux[at],
                        jnp.maximum(here, there) - self.r_base[at],
                        there - here,
                        self.r_fric[at],
                        self.r_drive[at],
                    )
                    flux[at] = out
                    self.total[at] += here
                    if j:
                        level[at] = (
                            here
                            - rate * (here - self.sur[at])
                            + (last_flux - out) * self.r_inv[at]
                        )
                    else:
                        first_flux = out
                    last_flux = out
                    here = there
                level[base] = (
                    first
                    - rate * (first - self.sur[base])
                    + (pltpu.roll(last_flux, 1, 0) - first_flux) * self.r_inv[base]
                )
            return carry

        lax.fori_loop(0, SUB, substep, 0)

    def floods(self, pairs):
        flood, _, q_east, q_north, _ = self.state
        for tiles in pairs:
            for j in range(self.sizes[tiles[0]]):
                norths = {t: q_north[self.base[t] + j] for t in tiles}
                for t in tiles:
                    base, size = self.base[t], self.sizes[t]
                    at = base + j
                    west = q_east[at - 1] if j else pltpu.roll(q_east[base + size - 1], 1, 0)
                    flooded = flood[at] + (TIME_STEP / CELL_SIZE) * (
                        west - q_east[at] + self.southward(norths.get, t) - norths[t]
                    )
                    flood[at] = flooded + self.give[at] * (self.total[at] - SUB * self.sur[at])


def fold(low, high):
    lane = lax.broadcasted_iota(jnp.int32, (8, LANES), 1)
    return jnp.where(lane < 64, pltpu.roll(low, 16, 1), high)


def exchange_kernel(
    n_lon,
    n_lat,
    depth_hbm,
    ground_hbm,
    rough_hbm,
    river_hbm,
    width_hbm,
    bank_hbm,
    mask_hbm,
    ext,
    sides,
    strips,
    corners,
    own_mask,
    inner,
    band,
    plain,
    floats,
    ints,
    mask_in,
    top,
    bottom,
    packed,
    relay,
    load_sem,
    send_sem,
    recv_sem,
    *scratch,
):
    lon = lax.axis_index("lon")
    lat = lax.axis_index("lat")
    east = lax.rem(lon + 1, n_lon)
    west = lax.rem(lon + n_lon - 1, n_lon)
    north = lax.rem(lat + 1, n_lat)
    south = lax.rem(lat + n_lat - 1, n_lat)
    around = [
        (east, lat),
        (west, lat),
        (lon, north),
        (lon, south),
    ]
    around = [{"lon": a, "lat": b} for a, b in around]
    barrier = pltpu.get_barrier_semaphore()
    for device in around:
        pl.semaphore_signal(barrier, inc=1, device_id=device, device_id_type=MESH)

    loads = []
    for number, (source, target) in enumerate(
        [
            (ground_hbm, floats.at[GROUND]),
            (bank_hbm, ints.at[0]),
            (width_hbm, ints.at[1]),
            (river_hbm, floats.at[RIVER]),
            (depth_hbm, floats.at[DEPTH]),
            (rough_hbm, floats.at[ROUGH]),
            (mask_hbm, mask_in),
        ]
    ):
        copy = pltpu.make_async_copy(source, target, load_sem.at[number])
        copy.start()
        loads.append(copy)

    def place(field, values):
        for tile in range(2):
            ext[field, tile, HALO : HALO + COLS, :] = values[tile * LANES : (tile + 1) * LANES, :].T
        top[field] = values[0:8, :]
        bottom[field] = values[ROWS - 8 : ROWS, :]

    loads[0].wait()
    ground = floats[GROUND]
    place(GROUND, ground)
    loads[1].wait()
    place(BED, ground - (1.0 + 0.5 * ints[0].astype(F32)))
    loads[2].wait()
    place(WIDTH, 8.0 + 9.0 * ints[1].astype(F32))
    loads[3].wait()
    place(RIVER, floats[RIVER])
    loads[4].wait()
    place(DEPTH, floats[DEPTH])
    loads[5].wait()
    place(ROUGH, floats[ROUGH])
    loads[6].wait()
    for tile in range(2):
        own_mask[tile] = jnp.broadcast_to(mask_in[tile : tile + 1, :].astype(F32), (8, LANES))
    top[6] = own_mask[0]
    bottom[6] = own_mask[1]
    sixteen = lax.broadcasted_iota(jnp.int32, (8, LANES), 1) // 16
    upper_mask = pltpu.roll(own_mask[0], 96, 1)
    lower_mask = pltpu.roll(own_mask[1], 112, 1)
    for side in range(2):
        for i in range(HALO // 8):
            at = 8 * i + (COLS if side else HALO)
            upper, lower = upper_mask, lower_mask
            for field in range(6):
                moved = ext[field, 0, at : at + 8, :]
                moved = pltpu.roll(moved, 16 * field, 1) if field else moved
                upper = jnp.where(sixteen == field, moved, upper)
                moved = pltpu.roll(ext[field, 1, at : at + 8, :], 16 * field + 16, 1)
                lower = jnp.where(sixteen == field, moved, lower)
            packed[side, 0, 8 * i : 8 * i + 8, :] = upper
            packed[side, 1, 8 * i : 8 * i + 8, :] = lower

    pl.semaphore_wait(barrier, len(around))
    fields = pl.ds(0, 6)
    both = pl.ds(0, 2)
    sends = [
        (packed.at[1], relay.at[0], around[0]),
        (packed.at[0], relay.at[1], around[1]),
        (
            ext.at[fields, both, pl.ds(COLS, HALO), :],
            ext.at[fields, both, pl.ds(0, HALO), :],
            around[0],
        ),
        (
            ext.at[fields, both, pl.ds(HALO, HALO), :],
            ext.at[fields, both, pl.ds(HALO + COLS, HALO), :],
            around[1],
        ),
        (bottom, strips.at[FROM_S], around[2]),
        (top, strips.at[FROM_N], around[3]),
        (own_mask, sides.at[0], around[0]),
        (own_mask, sides.at[1], around[1]),
    ]
    copies = []

    def send(source, target, device):
        number = len(copies)
        copy = pltpu.make_async_remote_copy(
            src_ref=source,
            dst_ref=target,
            send_sem=send_sem.at[number],
            recv_sem=recv_sem.at[number],
            device_id=device,
            device_id_type=MESH,
        )
        copy.start()
        copies.append(copy)

    for source, target, device in sends:
        send(source, target, device)

    size = COLS // 8
    zone = Zone(scratch, [size, size], [1, 0])
    for tile in range(2):
        def load(field, j):
            return ext[field, tile, pl.ds(HALO + j, 8, stride=size), :]

        zone.prepare(tile, load, lambda c: c == COLS - 1, lambda c: own_mask[tile])
        zone.begin(tile, load)
    pairs = [(0, 1)]
    zone.prepare_north((0, 1))
    drives = [DRIVE, jnp.where((zone.lane == LANES - 1) & (lat == n_lat - 1), 0.0, DRIVE)]

    def step(number, carry):
        zone.flows(pairs, drives)
        zone.rivers()
        zone.floods(pairs)
        for k in range(STATE):
            for tile in range(2):
                for j in range(size):
                    inner[number, k, tile, pl.ds(j, 8, stride=size), :] = zone.state[k][
                        zone.base[tile] + j
                    ]
        return carry

    lax.fori_loop(0, STEPS, step, 0)

    for side in (1, 0):
        copies[side].wait()
        where = pl.ds(HALO * side, HALO)
        send(relay.at[side, 1], corners.at[FROM_S, where], around[2])
        send(relay.at[side, 0], corners.at[FROM_N, where], around[3])

    for field in range(6):
        values = [
            fold(
                ext[field, 0, HALO + 8 * i : HALO + 8 * i + 8, :],
                ext[field, 1, HALO + 8 * i : HALO + 8 * i + 8, :],
            )
            for i in range(size)
        ]
        for i in range(BAND // 8):
            value = jnp.ones((8, LANES), F32)
            for k in range(4):
                at = 4 * k - 4 + i
                if 0 <= at < size:
                    moved = pltpu.roll(values[at], (32 * k + 8) % LANES, 1)
                    value = jnp.where(zone.lane // 32 == k, moved, value)
            band[field, 8 * i : 8 * i + 8, :] = value

    for number in (2, 3, 6, 7):
        copies[number].wait()
    zero = jnp.zeros((STRIPS[0], LANES), F32)
    for side in range(2):
        at = pl.ds((WIDE - STRIPS[0]) * side, STRIPS[0])
        for tile in range(2):
            plain[FLOOD, tile, at, :] = ext[DEPTH, tile, at, :]
            plain[LEVEL, tile, at, :] = ext[BED, tile, at, :] + ext[RIVER, tile, at, :]
            for k in (EAST, NORTH, FLUX):
                plain[k, tile, at, :] = zero

    def strip_step(step, shift, strip):
        size = strip // 8
        zone = Zone(scratch, [size] * 4, [1, 0, 3, 2])
        pairs = [(0, 1), (2, 3)]
        starts = (shift, WIDE - strip - shift)
        for side in range(2):
            start = starts[side]
            for tile in range(2):
                t = 2 * side + tile

                def load(field, j):
                    return ext[field, tile, pl.ds(start + j, 8, stride=size), :]

                zone.prepare(
                    t,
                    load,
                    lambda c: (c + start == HALO - 1)
                    | (c + start == HALO + COLS - 1)
                    | (c == strip - 1),
                    lambda c: jnp.where(
                        (c + start < HALO) if side == 0 else (c + start >= HALO + COLS),
                        sides[side, tile],
                        own_mask[tile],
                    ),
                )
                for k in range(STATE):
                    for j in range(size):
                        zone.state[k][zone.base[t] + j] = plain[
                            k, tile, pl.ds(start + j, 8, stride=size), :
                        ]
            zone.prepare_north((2 * side, 2 * side + 1))
        zone.flows(pairs, [drives[0], drives[1], drives[0], drives[1]])
        zone.rivers()
        zone.floods(pairs)
        last = strip != STRIPS[0]
        for side in range(2):
            start = starts[side]
            for tile in range(2):
                t = 2 * side + tile
                for k in range(4 if last else STATE):
                    for j in range(size):
                        plain[k, tile, pl.ds(start + j, 8, stride=size), :] = zone.state[k][
                            zone.base[t] + j
                        ]
                    if last:
                        continue
                    for part in range(2):
                        at = pl.multiple_of(
                            8 * step + 8 * part if side == 0 else 112 - 8 * step + 8 * part, 8
                        )
                        value = inner[step, k, tile, pl.ds(at, 8), :]
                        if part == side and k in (FLOOD, EAST):
                            old = plain[k, tile, pl.ds(HALO + at, 8), :]
                            kept = (zone.sublane == (7 if side else 0)) & (step == 0)
                            value = jnp.where(kept, old, value)
                        plain[k, tile, pl.ds(HALO + at, 8), :] = value

    for step in range(STEPS - 1):
        strip_step(step, 8 * step, STRIPS[0])
    strip_step(STEPS - 1, 16, STRIPS[1])
    for number in (4, 5, 8, 9, 10, 11):
        copies[number].wait()


def flow_kernel(
    n_lat,
    ext,
    sides,
    strips,
    corners,
    own_mask,
    inner,
    band,
    plain,
    flood_out,
    river_out,
    east_out,
    north_out,
    rows,
    ends,
    stage,
    sems,
    *scratch,
):
    lat = lax.axis_index("lat")
    wide = BAND // 8
    zone = Zone(scratch, [wide], [0])
    lane, sublane = zone.lane, zone.sublane
    group, place = lane // 32, lane % 32
    halo_lane = (place >= 8) & (place < 24)
    pairs = [(0,)]
    row_closed = ((place == 7) & (lat == n_lat - 1)) | ((place == 23) & (lat == 0))
    drives = [jnp.where(row_closed, 0.0, DRIVE)]
    outs = (flood_out, river_out, east_out, north_out)

    copies = []
    for k in (EAST, NORTH, FLOOD, LEVEL):
        for tile in range(2):
            pieces = []
            for i in range(COLS // 8):
                if 3 <= i < 13:
                    value = inner[STEPS - 1, k, tile, 8 * i : 8 * i + 8, :]
                else:
                    value = plain[k, tile, HALO + 8 * i : HALO + 8 * i + 8, :]
                if k == LEVEL:
                    at = HALO + 8 * i
                    value = jnp.where(
                        own_mask[tile] > 0.0,
                        value - ext[BED, tile, at : at + 8, :],
                        ext[RIVER, tile, at : at + 8, :],
                    )
                pieces.append(value)
            stage[k, tile * LANES : (tile + 1) * LANES, :] = jnp.concatenate(pieces, axis=0).T
        body_rows = pl.ds(8, ROWS - 16)
        copy = pltpu.make_async_copy(stage.at[k, body_rows], outs[k].at[body_rows], sems.at[k])
        copy.start()
        copies.append(copy)

    ones = jnp.ones((8, LANES), F32)
    joined = [
        jnp.where(
            lane % 16 < 8,
            corners[FROM_N, 8 * i : 8 * i + 8, :],
            corners[FROM_S, 8 * i : 8 * i + 8, :],
        )
        for i in range(2 * HALO // 8)
    ]
    for field in range(6):
        pieces = []
        for k in range(4):
            pieces.append(ones)
            for which in (FROM_N, FROM_S):
                value = strips[which, field]
                if k != 1:
                    value = pltpu.roll(value, (160 - 32 * k) % LANES, 1)
                pieces.append(value)
            pieces.append(ones)
        block = jnp.concatenate(pieces, axis=0).T
        for i in range(wide):
            value = band[field, 8 * i : 8 * i + 8, :]
            halo = block[8 * i : 8 * i + 8, :]
            for side, first in ((0, 1), (1, 8)):
                if first <= i < first + 3:
                    ours = group == 3 * side
                    at = 8 * (i - first)
                    moved = pltpu.roll(
                        joined[i - first + 3 * side], (8 + 96 * side - 16 * field) % LANES, 1
                    )
                    halo = jnp.where(ours, moved, halo)
                    at += (HALO + COLS) * side
                    moved = fold(ext[field, 0, at : at + 8, :], ext[field, 1, at : at + 8, :])
                    value = jnp.where(ours, pltpu.roll(moved, 8 + 96 * side, 1), value)
            rows[field, 8 * i : 8 * i + 8, :] = jnp.where(halo_lane, halo, value)

    def row_mask(low, high, halo):
        value = jnp.where(place < 8, pltpu.roll(high, 8, 1), pltpu.roll(low, 24, 1))
        return jnp.where(halo_lane, halo, value)

    middle = row_mask(
        own_mask[0],
        own_mask[1],
        jnp.where(
            place < 16, pltpu.roll(strips[FROM_N, 6], 8, 1), pltpu.roll(strips[FROM_S, 6], 24, 1)
        ),
    )
    west = row_mask(sides[0, 0], sides[0, 1], pltpu.roll(joined[0], 40, 1))
    east = row_mask(sides[1, 0], sides[1, 1], pltpu.roll(joined[3], 40, 1))
    east = pltpu.roll(east, 96, 1)
    spread = middle
    for k in range(1, 4):
        spread = jnp.where(group == k, pltpu.roll(middle, 32 * k, 1), spread)

    def load_row(field, j):
        return rows[field, pl.ds(j, 8, stride=wide), :]

    zone.prepare(
        0,
        load_row,
        lambda c: ((c == 31) & (group == 0)) | ((c == 63) & (group == 3)) | (c == BAND - 1),
        lambda c: jnp.where(
            (c < 32) & (group == 0), west, jnp.where((c >= 64) & (group == 3), east, spread)
        ),
    )
    zone.begin(0, load_row)
    zone.prepare_north((0,))

    def step(_, carry):
        zone.flows(pairs, drives)
        zone.rivers()
        zone.floods(pairs)
        return carry

    for _ in range(STEPS):
        step(_, 0)

    for k in range(4):
        for j in range(wide):
            ends[k, pl.ds(j, 8, stride=wide), :] = zone.state[k][zone.base[0] + j]
    pieces = []
    for k in range(4):
        for at in range(32, 64, 8):
            value = ends[k, at : at + 8, :]
            if k == LEVEL:
                value = jnp.where(
                    spread > 0.0,
                    value - rows[BED, at : at + 8, :],
                    rows[RIVER, at : at + 8, :],
                )
            pieces.append(value)
    turned = jnp.concatenate(pieces, axis=0).T
    for k in range(4):
        for which in range(2):
            value = None
            for g in range(4):
                at = 32 * g + (24 if which == 0 else 0)
                piece = turned[at : at + 8, :]
                shift = (32 * g - 32 * k) % LANES
                piece = pltpu.roll(piece, shift, 1) if shift else piece
                value = piece if value is None else jnp.where(group == g, piece, value)
            first = 0 if which == 0 else ROWS - 8
            taken = (sublane < 4) if which == 0 else (sublane >= 4)
            end_rows = pl.ds(first, 8)
            stage[k, end_rows, :] = jnp.where(taken, value, stage[k, end_rows, :])
            copy = pltpu.make_async_copy(
                stage.at[k, end_rows], outs[k].at[end_rows], sems.at[4 + 2 * k + which]
            )
            copy.start()
            copies.append(copy)
    for copy in copies:
        copy.wait()


def body(n_lon, n_lat, depth_init, ground, roughness, river_init, reach_mask, width_class, bank_class):
    mask = reach_mask.reshape(2, LANES)
    field = (ROWS, COLS)
    far = pl.BlockSpec(memory_space=pltpu.HBM)
    near = pl.BlockSpec(memory_space=pltpu.VMEM)
    state = [pltpu.VMEM((REGISTERS, 8, LANES), F32)] * SCRATCH
    handed = pl.pallas_call(
        functools.partial(exchange_kernel, n_lon, n_lat),
        out_shape=(
            pltpu.VMEM((6, 2, WIDE, LANES), F32),
            pltpu.VMEM((2, 2, 8, LANES), F32),
            pltpu.VMEM((2, 7, 8, LANES), F32),
            pltpu.VMEM((2, 2 * HALO, LANES), F32),
            pltpu.VMEM((2, 8, LANES), F32),
            pltpu.VMEM((STEPS, STATE, 2, COLS, LANES), F32),
            pltpu.VMEM((6, BAND, LANES), F32),
            pltpu.VMEM((STATE, 2, WIDE, LANES), F32),
        ),
        in_specs=[far] * 7,
        out_specs=(near,) * 8,
        scratch_shapes=[
            pltpu.VMEM((4, ROWS, COLS), F32),
            pltpu.VMEM((2, ROWS, COLS), jnp.int32),
            pltpu.VMEM((2, LANES), jnp.int32),
            pltpu.VMEM((7, 8, LANES), F32),
            pltpu.VMEM((7, 8, LANES), F32),
            pltpu.VMEM((2, 2, HALO, LANES), F32),
            pltpu.VMEM((2, 2, HALO, LANES), F32),
            pltpu.SemaphoreType.DMA((7,)),
            pltpu.SemaphoreType.DMA((12,)),
            pltpu.SemaphoreType.DMA((12,)),
        ]
        + state,
        compiler_params=pltpu.CompilerParams(
            collective_id=0, has_side_effects=True, vmem_limit_bytes=VMEM_LIMIT
        ),
        name="exchange",
    )(*[
        pltpu.with_memory_space_constraint(x, pltpu.HBM)
        for x in (depth_init, ground, roughness, river_init, width_class, bank_class, mask)
    ])
    handed = [pltpu.with_memory_space_constraint(x, pltpu.VMEM) for x in handed]
    return pl.pallas_call(
        functools.partial(flow_kernel, n_lat),
        out_shape=(jax.ShapeDtypeStruct(field, F32),) * 4,
        in_specs=[near] * 8,
        out_specs=(far,) * 4,
        scratch_shapes=[
            pltpu.VMEM((6, BAND, LANES), F32),
            pltpu.VMEM((4, BAND, LANES), F32),
            pltpu.VMEM((4, ROWS, COLS), F32),
            pltpu.SemaphoreType.DMA((12,)),
        ]
        + state,
        compiler_params=pltpu.CompilerParams(vmem_limit_bytes=VMEM_LIMIT),
        name="flow",
    )(*handed)


def solution(mesh):
    placed = P("lat", "lon")
    return jax.shard_map(
        functools.partial(body, mesh.shape["lon"], mesh.shape["lat"]),
        mesh=mesh,
        in_specs=(placed,) * 7,
        out_specs=(placed,) * 4,
        check_vma=False,
    )
```

```python
import functools
import math

import jax
import jax.numpy as jnp
from jax import lax
from jax.experimental import pallas as pl
from jax.experimental.pallas import tpu as pltpu
from jax.sharding import PartitionSpec as P

MESH = pl.DeviceIdType.MESH
F32 = jnp.float32
SUB = 8
STEPS = 4
ROWS = 256
COLS = 128
HALO = 24
WIDE = COLS + 2 * HALO
LANES = 128
STRIPS = (32, 40)
BAND = 96
DEPTH, GROUND, ROUGH, RIVER, WIDTH, BED = range(6)
FROM_S, FROM_N = range(2)
FLOOD, LEVEL, EAST, NORTH, FLUX = range(5)

GRAVITY = 9.81
CELL_SIZE = 90.0
TIME_STEP = 10.0
SHALLOW = 0.1
EXCHANGE = 0.01
CHANNEL_MANNING = 0.035
SHORT_STEP = TIME_STEP / SUB
POWER = -7.0 / 6.0 / math.log(2.0)
DRIVE = GRAVITY * TIME_STEP / CELL_SIZE

STATE = 5
SCRATCH = 17
REGISTERS = 32
UNROLL = 8
VMEM_LIMIT = 24 << 20


def quotient(current, height, drop, friction, drive):
    power = jnp.exp2(POWER * jnp.log(height * height + SHALLOW * SHALLOW))
    resisted = 1.0 + friction * jnp.abs(current) * power
    return (current - drive * (height * drop)) / resisted


class Zone:
    def __init__(self, refs, sizes, partners):
        self.sizes = sizes
        self.partners = partners
        self.base = [sum(sizes[:t]) for t in range(len(sizes))]
        self.state = refs[:STATE]
        (
            self.g,
            self.sur,
            self.e_base,
            self.e_fric,
            self.n_base,
            self.n_fric,
            self.r_base,
            self.r_drive,
            self.r_fric,
            self.r_inv,
            self.give,
            self.total,
        ) = refs[STATE:]
        self.lane = lax.broadcasted_iota(jnp.int32, (8, LANES), 1)
        self.sublane = lax.broadcasted_iota(jnp.int32, (8, LANES), 0)

    def column(self, tile, j):
        return self.sublane * self.sizes[tile] + j

    def northward(self, read, tile):
        here = pltpu.roll(read(tile), LANES - 1, 1)
        if self.partners[tile] == tile:
            return here
        there = pltpu.roll(read(self.partners[tile]), LANES - 1, 1)
        return jnp.where(self.lane == LANES - 1, there, here)

    def southward(self, read, tile):
        here = pltpu.roll(read(tile), 1, 1)
        if self.partners[tile] == tile:
            return here
        there = pltpu.roll(read(self.partners[tile]), 1, 1)
        return jnp.where(self.lane == 0, there, here)

    def prepare(self, tile, load, closed, mask):
        size, base = self.sizes[tile], self.base[tile]

        def after(values, j):
            return values[j + 1] if j + 1 < size else pltpu.roll(values[0], 7, 0)

        grounds = [load(GROUND, j) for j in range(size)]
        roughs = [load(ROUGH, j) for j in range(size)]
        beds = [load(BED, j) for j in range(size)]
        widths = [load(WIDTH, j) for j in range(size)]
        for j in range(size):
            at = base + j
            column = self.column(tile, j)
            self.g[at] = grounds[j]
            self.e_base[at] = jnp.maximum(grounds[j], after(grounds, j))
            self.e_fric[at] = (GRAVITY * TIME_STEP) * (roughs[j] * after(roughs, j))
            self.n_fric[at] = roughs[j]
            breadth = 0.5 * (widths[j] + after(widths, j))
            self.r_base[at] = jnp.maximum(beds[j], after(beds, j))
            self.r_drive[at] = jnp.where(
                closed(column), 0.0, (GRAVITY * SHORT_STEP / CELL_SIZE) * breadth
            )
            self.r_fric[at] = (
                GRAVITY * SHORT_STEP * CHANNEL_MANNING * CHANNEL_MANNING
            ) / breadth
            self.r_inv[at] = SHORT_STEP / (CELL_SIZE * widths[j])
            self.give[at] = mask(column) * widths[j] * (SHORT_STEP * EXCHANGE / CELL_SIZE)

    def prepare_north(self, tiles):
        for j in range(self.sizes[tiles[0]]):
            grounds = {t: self.g[self.base[t] + j] for t in tiles}
            roughs = {t: self.n_fric[self.base[t] + j] for t in tiles}
            for t in tiles:
                at = self.base[t] + j
                self.n_base[at] = jnp.maximum(grounds[t], self.northward(grounds.get, t))
                self.n_fric[at] = (GRAVITY * TIME_STEP) * (
                    roughs[t] * self.northward(roughs.get, t)
                )

    def begin(self, tile, load):
        for j in range(self.sizes[tile]):
            at = self.base[tile] + j
            self.state[FLOOD][at] = load(DEPTH, j)
            self.state[LEVEL][at] = load(BED, j) + load(RIVER, j)
            for k in (EAST, NORTH, FLUX):
                self.state[k][at] = jnp.zeros((8, LANES), F32)

    def flows(self, pairs, drives):
        flood, _, q_east, q_north, _ = self.state
        for tiles in pairs:
            for t in tiles:
                for j in range(self.sizes[t]):
                    at = self.base[t] + j
                    self.sur[at] = self.g[at] + flood[at]
                    self.total[at] = jnp.zeros((8, LANES), F32)
        for tiles in pairs:
            for t in tiles:
                base, size = self.base[t], self.sizes[t]
                for j in range(size):
                    here = self.sur[base + j]
                    there = (
                        self.sur[base + j + 1] if j + 1 < size else pltpu.roll(self.sur[base], 7, 0)
                    )
                    q_east[base + j] = quotient(
                        q_east[base + j],
                        jnp.maximum(here, there) - self.e_base[base + j],
                        there - here,
                        self.e_fric[base + j],
                        DRIVE,
                    )
        for tiles in pairs:
            for j in range(self.sizes[tiles[0]]):
                surfaces = {t: self.sur[self.base[t] + j] for t in tiles}
                for t in tiles:
                    at = self.base[t] + j
                    there = self.northward(surfaces.get, t)
                    q_north[at] = quotient(
                        q_north[at],
                        jnp.maximum(surfaces[t], there) - self.n_base[at],
                        there - surfaces[t],
                        self.n_fric[at],
                        drives[t],
                    )

    def rivers(self):
        level, flux = self.state[LEVEL], self.state[FLUX]
        rate = SHORT_STEP * EXCHANGE

        if sum(self.sizes) > 20:
            return self.rivers_in_memory()
        count = sum(self.sizes)

        def substep(_, carry):
            levels, fluxes = list(carry[:count]), list(carry[count:])
            outs = [None] * count
            for t, size in enumerate(self.sizes):
                base = self.base[t]
                for j in range(size):
                    at = base + j
                    here = levels[at]
                    there = levels[at + 1] if j + 1 < size else pltpu.roll(levels[base], 7, 0)
                    outs[at] = quotient(
                        fluxes[at],
                        jnp.maximum(here, there) - self.r_base[at],
                        there - here,
                        self.r_fric[at],
                        self.r_drive[at],
                    )
                    self.total[at] += here
            fresh = []
            for t, size in enumerate(self.sizes):
                base = self.base[t]
                for j in range(size):
                    at = base + j
                    west = outs[at - 1] if j else pltpu.roll(outs[base + size - 1], 1, 0)
                    fresh.append(
                        (1.0 - rate) * levels[at]
                        + (rate * self.sur[at] + (west - outs[at]) * self.r_inv[at])
                    )
            return tuple(fresh) + tuple(outs)

        start = [level[at] for at in range(count)] + [flux[at] for at in range(count)]
        final = lax.fori_loop(0, SUB, substep, tuple(start), unroll=UNROLL)
        for at in range(count):
            level[at] = final[at]
            flux[at] = final[count + at]

    def rivers_in_memory(self):
        level, flux = self.state[LEVEL], self.state[FLUX]
        rate = SHORT_STEP * EXCHANGE

        def substep(_, carry):
            for t, size in enumerate(self.sizes):
                base = self.base[t]
                first = level[base]
                here = first
                first_flux = None
                last_flux = None
                for j in range(size):
                    at = base + j
                    there = level[at + 1] if j + 1 < size else pltpu.roll(first, 7, 0)
                    out = quotient(
                        flux[at],
                        jnp.maximum(here, there) - self.r_base[at],
                        there - here,
                        self.r_fric[at],
                        self.r_drive[at],
                    )
                    flux[at] = out
                    self.total[at] += here
                    if j:
                        level[at] = (
                            here
                            - rate * (here - self.sur[at])
                            + (last_flux - out) * self.r_inv[at]
                        )
                    else:
                        first_flux = out
                    last_flux = out
                    here = there
                level[base] = (
                    first
                    - rate * (first - self.sur[base])
                    + (pltpu.roll(last_flux, 1, 0) - first_flux) * self.r_inv[base]
                )
            return carry

        lax.fori_loop(0, SUB, substep, 0, unroll=2)

    def floods(self, pairs):
        flood, _, q_east, q_north, _ = self.state
        for tiles in pairs:
            for j in range(self.sizes[tiles[0]]):
                norths = {t: q_north[self.base[t] + j] for t in tiles}
                for t in tiles:
                    base, size = self.base[t], self.sizes[t]
                    at = base + j
                    west = q_east[at - 1] if j else pltpu.roll(q_east[base + size - 1], 1, 0)
                    flooded = flood[at] + (TIME_STEP / CELL_SIZE) * (
                        west - q_east[at] + self.southward(norths.get, t) - norths[t]
                    )
                    flood[at] = flooded + self.give[at] * (self.total[at] - SUB * self.sur[at])


def fold(low, high):
    lane = lax.broadcasted_iota(jnp.int32, (8, LANES), 1)
    return jnp.where(lane < 64, pltpu.roll(low, 16, 1), high)


def exchange_kernel(
    n_lon,
    n_lat,
    depth_hbm,
    ground_hbm,
    rough_hbm,
    river_hbm,
    width_hbm,
    bank_hbm,
    mask_hbm,
    ext,
    sides,
    strips,
    corners,
    own_mask,
    inner,
    band,
    plain,
    floats,
    ints,
    mask_in,
    top,
    bottom,
    packed,
    relay,
    load_sem,
    send_sem,
    recv_sem,
    *scratch,
):
    lon = lax.axis_index("lon")
    lat = lax.axis_index("lat")
    east = lax.rem(lon + 1, n_lon)
    west = lax.rem(lon + n_lon - 1, n_lon)
    north = lax.rem(lat + 1, n_lat)
    south = lax.rem(lat + n_lat - 1, n_lat)
    around = [
        (east, lat),
        (west, lat),
        (lon, north),
        (lon, south),
    ]
    around = [{"lon": a, "lat": b} for a, b in around]
    barrier = pltpu.get_barrier_semaphore()
    for device in around:
        pl.semaphore_signal(barrier, inc=1, device_id=device, device_id_type=MESH)

    loads = []
    for number, (source, target) in enumerate(
        [
            (ground_hbm, floats.at[GROUND]),
            (bank_hbm, ints.at[0]),
            (width_hbm, ints.at[1]),
            (river_hbm, floats.at[RIVER]),
            (depth_hbm, floats.at[DEPTH]),
            (rough_hbm, floats.at[ROUGH]),
            (mask_hbm, mask_in),
        ]
    ):
        copy = pltpu.make_async_copy(source, target, load_sem.at[number])
        copy.start()
        loads.append(copy)

    def place(field, values):
        for tile in range(2):
            ext[field, tile, HALO : HALO + COLS, :] = values[tile * LANES : (tile + 1) * LANES, :].T
        top[field] = values[0:8, :]
        bottom[field] = values[ROWS - 8 : ROWS, :]

    loads[0].wait()
    ground = floats[GROUND]
    place(GROUND, ground)
    loads[1].wait()
    place(BED, ground - (1.0 + 0.5 * ints[0].astype(F32)))
    loads[2].wait()
    place(WIDTH, 8.0 + 9.0 * ints[1].astype(F32))
    loads[3].wait()
    place(RIVER, floats[RIVER])
    loads[4].wait()
    place(DEPTH, floats[DEPTH])
    loads[5].wait()
    place(ROUGH, floats[ROUGH])
    loads[6].wait()
    for tile in range(2):
        own_mask[tile] = jnp.broadcast_to(mask_in[tile : tile + 1, :].astype(F32), (8, LANES))
    top[6] = own_mask[0]
    bottom[6] = own_mask[1]
    sixteen = lax.broadcasted_iota(jnp.int32, (8, LANES), 1) // 16
    upper_mask = pltpu.roll(own_mask[0], 96, 1)
    lower_mask = pltpu.roll(own_mask[1], 112, 1)
    for side in range(2):
        for i in range(HALO // 8):
            at = 8 * i + (COLS if side else HALO)
            upper, lower = upper_mask, lower_mask
            for field in range(6):
                moved = ext[field, 0, at : at + 8, :]
                moved = pltpu.roll(moved, 16 * field, 1) if field else moved
                upper = jnp.where(sixteen == field, moved, upper)
                moved = pltpu.roll(ext[field, 1, at : at + 8, :], 16 * field + 16, 1)
                lower = jnp.where(sixteen == field, moved, lower)
            packed[side, 0, 8 * i : 8 * i + 8, :] = upper
            packed[side, 1, 8 * i : 8 * i + 8, :] = lower

    pl.semaphore_wait(barrier, len(around))
    fields = pl.ds(0, 6)
    both = pl.ds(0, 2)
    sends = [
        (packed.at[1], relay.at[0], around[0]),
        (packed.at[0], relay.at[1], around[1]),
        (
            ext.at[fields, both, pl.ds(COLS, HALO), :],
            ext.at[fields, both, pl.ds(0, HALO), :],
            around[0],
        ),
        (
            ext.at[fields, both, pl.ds(HALO, HALO), :],
            ext.at[fields, both, pl.ds(HALO + COLS, HALO), :],
            around[1],
        ),
        (bottom, strips.at[FROM_S], around[2]),
        (top, strips.at[FROM_N], around[3]),
        (own_mask, sides.at[0], around[0]),
        (own_mask, sides.at[1], around[1]),
    ]
    copies = []

    def send(source, target, device):
        number = len(copies)
        copy = pltpu.make_async_remote_copy(
            src_ref=source,
            dst_ref=target,
            send_sem=send_sem.at[number],
            recv_sem=recv_sem.at[number],
            device_id=device,
            device_id_type=MESH,
        )
        copy.start()
        copies.append(copy)

    for source, target, device in sends:
        send(source, target, device)

    size = COLS // 8
    zone = Zone(scratch, [size, size], [1, 0])
    for tile in range(2):
        def load(field, j):
            return ext[field, tile, pl.ds(HALO + j, 8, stride=size), :]

        zone.prepare(tile, load, lambda c: c == COLS - 1, lambda c: own_mask[tile])
        zone.begin(tile, load)
    pairs = [(0, 1)]
    zone.prepare_north((0, 1))
    drives = [DRIVE, jnp.where((zone.lane == LANES - 1) & (lat == n_lat - 1), 0.0, DRIVE)]

    def step(number, carry):
        zone.flows(pairs, drives)
        zone.rivers()
        zone.floods(pairs)
        for k in range(STATE):
            for tile in range(2):
                for j in range(size):
                    inner[number, k, tile, pl.ds(j, 8, stride=size), :] = zone.state[k][
                        zone.base[tile] + j
                    ]
        return carry

    lax.fori_loop(0, STEPS, step, 0)

    for side in (1, 0):
        copies[side].wait()
        where = pl.ds(HALO * side, HALO)
        send(relay.at[side, 1], corners.at[FROM_S, where], around[2])
        send(relay.at[side, 0], corners.at[FROM_N, where], around[3])

    for field in range(6):
        values = [
            fold(
                ext[field, 0, HALO + 8 * i : HALO + 8 * i + 8, :],
                ext[field, 1, HALO + 8 * i : HALO + 8 * i + 8, :],
            )
            for i in range(size)
        ]
        for i in range(BAND // 8):
            value = jnp.ones((8, LANES), F32)
            for k in range(4):
                at = 4 * k - 4 + i
                if 0 <= at < size:
                    moved = pltpu.roll(values[at], (32 * k + 8) % LANES, 1)
                    value = jnp.where(zone.lane // 32 == k, moved, value)
            band[field, 8 * i : 8 * i + 8, :] = value

    for number in (2, 3, 6, 7):
        copies[number].wait()
    zero = jnp.zeros((STRIPS[0], LANES), F32)
    for side in range(2):
        at = pl.ds((WIDE - STRIPS[0]) * side, STRIPS[0])
        for tile in range(2):
            plain[FLOOD, tile, at, :] = ext[DEPTH, tile, at, :]
            plain[LEVEL, tile, at, :] = ext[BED, tile, at, :] + ext[RIVER, tile, at, :]
            for k in (EAST, NORTH, FLUX):
                plain[k, tile, at, :] = zero

    def strip_step(step, shift, strip):
        size = strip // 8
        zone = Zone(scratch, [size] * 4, [1, 0, 3, 2])
        pairs = [(0, 1), (2, 3)]
        starts = (shift, WIDE - strip - shift)
        for side in range(2):
            start = starts[side]
            for tile in range(2):
                t = 2 * side + tile

                def load(field, j):
                    return ext[field, tile, pl.ds(start + j, 8, stride=size), :]

                zone.prepare(
                    t,
                    load,
                    lambda c: (c + start == HALO - 1)
                    | (c + start == HALO + COLS - 1)
                    | (c == strip - 1),
                    lambda c: jnp.where(
                        (c + start < HALO) if side == 0 else (c + start >= HALO + COLS),
                        sides[side, tile],
                        own_mask[tile],
                    ),
                )
                for k in range(STATE):
                    for j in range(size):
                        zone.state[k][zone.base[t] + j] = plain[
                            k, tile, pl.ds(start + j, 8, stride=size), :
                        ]
            zone.prepare_north((2 * side, 2 * side + 1))
        zone.flows(pairs, [drives[0], drives[1], drives[0], drives[1]])
        zone.rivers()
        zone.floods(pairs)
        last = strip != STRIPS[0]
        for side in range(2):
            start = starts[side]
            for tile in range(2):
                t = 2 * side + tile
                for k in range(4 if last else STATE):
                    for j in range(size):
                        plain[k, tile, pl.ds(start + j, 8, stride=size), :] = zone.state[k][
                            zone.base[t] + j
                        ]
                    if last:
                        continue
                    for part in range(2):
                        at = pl.multiple_of(
                            8 * step + 8 * part if side == 0 else 112 - 8 * step + 8 * part, 8
                        )
                        value = inner[step, k, tile, pl.ds(at, 8), :]
                        if part == side and k in (FLOOD, EAST):
                            old = plain[k, tile, pl.ds(HALO + at, 8), :]
                            kept = (zone.sublane == (7 if side else 0)) & (step == 0)
                            value = jnp.where(kept, old, value)
                        plain[k, tile, pl.ds(HALO + at, 8), :] = value

    for step in range(STEPS - 1):
        strip_step(step, 8 * step, STRIPS[0])
    strip_step(STEPS - 1, 16, STRIPS[1])
    for number in (4, 5, 8, 9, 10, 11):
        copies[number].wait()


def flow_kernel(
    n_lat,
    ext,
    sides,
    strips,
    corners,
    own_mask,
    inner,
    band,
    plain,
    flood_out,
    river_out,
    east_out,
    north_out,
    rows,
    ends,
    stage,
    sems,
    *scratch,
):
    lat = lax.axis_index("lat")
    wide = BAND // 8
    zone = Zone(scratch, [wide], [0])
    lane, sublane = zone.lane, zone.sublane
    group, place = lane // 32, lane % 32
    halo_lane = (place >= 8) & (place < 24)
    pairs = [(0,)]
    row_closed = ((place == 7) & (lat == n_lat - 1)) | ((place == 23) & (lat == 0))
    drives = [jnp.where(row_closed, 0.0, DRIVE)]
    outs = (flood_out, river_out, east_out, north_out)

    copies = []
    for k in (EAST, NORTH, FLOOD, LEVEL):
        for tile in range(2):
            pieces = []
            for i in range(COLS // 8):
                if 3 <= i < 13:
                    value = inner[STEPS - 1, k, tile, 8 * i : 8 * i + 8, :]
                else:
                    value = plain[k, tile, HALO + 8 * i : HALO + 8 * i + 8, :]
                if k == LEVEL:
                    at = HALO + 8 * i
                    value = jnp.where(
                        own_mask[tile] > 0.0,
                        value - ext[BED, tile, at : at + 8, :],
                        ext[RIVER, tile, at : at + 8, :],
                    )
                pieces.append(value)
            stage[k, tile * LANES : (tile + 1) * LANES, :] = jnp.concatenate(pieces, axis=0).T
        body_rows = pl.ds(8, ROWS - 16)
        copy = pltpu.make_async_copy(stage.at[k, body_rows], outs[k].at[body_rows], sems.at[k])
        copy.start()
        copies.append(copy)

    ones = jnp.ones((8, LANES), F32)
    joined = [
        jnp.where(
            lane % 16 < 8,
            corners[FROM_N, 8 * i : 8 * i + 8, :],
            corners[FROM_S, 8 * i : 8 * i + 8, :],
        )
        for i in range(2 * HALO // 8)
    ]
    for field in range(6):
        pieces = []
        for k in range(4):
            pieces.append(ones)
            for which in (FROM_N, FROM_S):
                value = strips[which, field]
                if k != 1:
                    value = pltpu.roll(value, (160 - 32 * k) % LANES, 1)
                pieces.append(value)
            pieces.append(ones)
        block = jnp.concatenate(pieces, axis=0).T
        for i in range(wide):
            value = band[field, 8 * i : 8 * i + 8, :]
            halo = block[8 * i : 8 * i + 8, :]
            for side, first in ((0, 1), (1, 8)):
                if first <= i < first + 3:
                    ours = group == 3 * side
                    at = 8 * (i - first)
                    moved = pltpu.roll(
                        joined[i - first + 3 * side], (8 + 96 * side - 16 * field) % LANES, 1
                    )
                    halo = jnp.where(ours, moved, halo)
                    at += (HALO + COLS) * side
                    moved = fold(ext[field, 0, at : at + 8, :], ext[field, 1, at : at + 8, :])
                    value = jnp.where(ours, pltpu.roll(moved, 8 + 96 * side, 1), value)
            rows[field, 8 * i : 8 * i + 8, :] = jnp.where(halo_lane, halo, value)

    def row_mask(low, high, halo):
        value = jnp.where(place < 8, pltpu.roll(high, 8, 1), pltpu.roll(low, 24, 1))
        return jnp.where(halo_lane, halo, value)

    middle = row_mask(
        own_mask[0],
        own_mask[1],
        jnp.where(
            place < 16, pltpu.roll(strips[FROM_N, 6], 8, 1), pltpu.roll(strips[FROM_S, 6], 24, 1)
        ),
    )
    west = row_mask(sides[0, 0], sides[0, 1], pltpu.roll(joined[0], 40, 1))
    east = row_mask(sides[1, 0], sides[1, 1], pltpu.roll(joined[3], 40, 1))
    east = pltpu.roll(east, 96, 1)
    spread = middle
    for k in range(1, 4):
        spread = jnp.where(group == k, pltpu.roll(middle, 32 * k, 1), spread)

    def load_row(field, j):
        return rows[field, pl.ds(j, 8, stride=wide), :]

    zone.prepare(
        0,
        load_row,
        lambda c: ((c == 31) & (group == 0)) | ((c == 63) & (group == 3)) | (c == BAND - 1),
        lambda c: jnp.where(
            (c < 32) & (group == 0), west, jnp.where((c >= 64) & (group == 3), east, spread)
        ),
    )
    zone.begin(0, load_row)
    zone.prepare_north((0,))

    def step(_, carry):
        zone.flows(pairs, drives)
        zone.rivers()
        zone.floods(pairs)
        return carry

    for _ in range(STEPS):
        step(_, 0)

    for k in range(4):
        for j in range(wide):
            ends[k, pl.ds(j, 8, stride=wide), :] = zone.state[k][zone.base[0] + j]
    pieces = []
    for k in range(4):
        for at in range(32, 64, 8):
            value = ends[k, at : at + 8, :]
            if k == LEVEL:
                value = jnp.where(
                    spread > 0.0,
                    value - rows[BED, at : at + 8, :],
                    rows[RIVER, at : at + 8, :],
                )
            pieces.append(value)
    turned = jnp.concatenate(pieces, axis=0).T
    for k in range(4):
        for which in range(2):
            value = None
            for g in range(4):
                at = 32 * g + (24 if which == 0 else 0)
                piece = turned[at : at + 8, :]
                shift = (32 * g - 32 * k) % LANES
                piece = pltpu.roll(piece, shift, 1) if shift else piece
                value = piece if value is None else jnp.where(group == g, piece, value)
            first = 0 if which == 0 else ROWS - 8
            taken = (sublane < 4) if which == 0 else (sublane >= 4)
            end_rows = pl.ds(first, 8)
            stage[k, end_rows, :] = jnp.where(taken, value, stage[k, end_rows, :])
            copy = pltpu.make_async_copy(
                stage.at[k, end_rows], outs[k].at[end_rows], sems.at[4 + 2 * k + which]
            )
            copy.start()
            copies.append(copy)
    for copy in copies:
        copy.wait()


def body(n_lon, n_lat, depth_init, ground, roughness, river_init, reach_mask, width_class, bank_class):
    mask = reach_mask.reshape(2, LANES)
    field = (ROWS, COLS)
    far = pl.BlockSpec(memory_space=pltpu.HBM)
    near = pl.BlockSpec(memory_space=pltpu.VMEM)
    state = [pltpu.VMEM((REGISTERS, 8, LANES), F32)] * SCRATCH
    handed = pl.pallas_call(
        functools.partial(exchange_kernel, n_lon, n_lat),
        out_shape=(
            pltpu.VMEM((6, 2, WIDE, LANES), F32),
            pltpu.VMEM((2, 2, 8, LANES), F32),
            pltpu.VMEM((2, 7, 8, LANES), F32),
            pltpu.VMEM((2, 2 * HALO, LANES), F32),
            pltpu.VMEM((2, 8, LANES), F32),
            pltpu.VMEM((STEPS, STATE, 2, COLS, LANES), F32),
            pltpu.VMEM((6, BAND, LANES), F32),
            pltpu.VMEM((STATE, 2, WIDE, LANES), F32),
        ),
        in_specs=[far] * 7,
        out_specs=(near,) * 8,
        scratch_shapes=[
            pltpu.VMEM((4, ROWS, COLS), F32),
            pltpu.VMEM((2, ROWS, COLS), jnp.int32),
            pltpu.VMEM((2, LANES), jnp.int32),
            pltpu.VMEM((7, 8, LANES), F32),
            pltpu.VMEM((7, 8, LANES), F32),
            pltpu.VMEM((2, 2, HALO, LANES), F32),
            pltpu.VMEM((2, 2, HALO, LANES), F32),
            pltpu.SemaphoreType.DMA((7,)),
            pltpu.SemaphoreType.DMA((12,)),
            pltpu.SemaphoreType.DMA((12,)),
        ]
        + state,
        compiler_params=pltpu.CompilerParams(
            collective_id=0, has_side_effects=True, vmem_limit_bytes=VMEM_LIMIT
        ),
        name="exchange",
    )(*[
        pltpu.with_memory_space_constraint(x, pltpu.HBM)
        for x in (depth_init, ground, roughness, river_init, width_class, bank_class, mask)
    ])
    handed = [pltpu.with_memory_space_constraint(x, pltpu.VMEM) for x in handed]
    return pl.pallas_call(
        functools.partial(flow_kernel, n_lat),
        out_shape=(jax.ShapeDtypeStruct(field, F32),) * 4,
        in_specs=[near] * 8,
        out_specs=(far,) * 4,
        scratch_shapes=[
            pltpu.VMEM((6, BAND, LANES), F32),
            pltpu.VMEM((4, BAND, LANES), F32),
            pltpu.VMEM((4, ROWS, COLS), F32),
            pltpu.SemaphoreType.DMA((12,)),
        ]
        + state,
        compiler_params=pltpu.CompilerParams(vmem_limit_bytes=VMEM_LIMIT),
        name="flow",
    )(*handed)


def solution(mesh):
    placed = P("lat", "lon")
    return jax.shard_map(
        functools.partial(body, mesh.shape["lon"], mesh.shape["lat"]),
        mesh=mesh,
        in_specs=(placed,) * 7,
        out_specs=(placed,) * 4,
        check_vma=False,
    )
```
